8 devices in a mesh: pp: 2 (over z, y), tp: 4 (over x, core).
Axes of the slice: x: 2, y: 2, z: 1, core: 2. Of those that a mesh axis runs over, the one named last changes fastest.
Arguments:
- activations: bfloat16 [256, 28, 28, 256], P(('pp', 'tp'))
- conv_w: bfloat16 [3, 3, 256, 256], P(None, None, 'tp')
- bn_scale: float32 [256], P('tp')
- bn_shift: float32 [256], P('tp')
Outputs:
- output: bfloat16 [256, 28, 28, 256], P('pp', None, None, 'tp')
All inputs are finite; a program needn't handle non-finite values.
Results may differ from the reference program's by a relative error of at most 0.001.
Values are sent between devices in bfloat16 or wider.
A program may use at most 1 GiB of HBM per device.

```python
import math
import jax
import jax.numpy as jnp
from jax import lax

IMAGES = 128
IMG_BLOCK = 128
HEIGHT = 28
WIDTH = 28
C_IN = 256
C_OUT = 256
CONV_DIMS = ("NHWC", "HWIO", "NHWC")


def setup_inputs(seed: int = 0) -> dict:
    base_key = jax.random.key(seed)
    act_key, w_key, scale_key, shift_key = jax.random.split(base_key, 4)
    live_rows = jax.random.normal(act_key, (IMAGES, HEIGHT, WIDTH, C_IN), jnp.float32)
    activations = jnp.concatenate([live_rows, jnp.zeros_like(live_rows)], axis=0).astype(jnp.bfloat16)
    w_scale = 1.0 / math.sqrt(9 * C_IN)
    conv_w = (jax.random.normal(w_key, (3, 3, C_IN, C_OUT), jnp.float32) * w_scale).astype(jnp.bfloat16)
    bn_scale = jax.random.uniform(scale_key, (C_OUT,), jnp.float32, 0.5, 1.5)
    bn_shift = 0.5 * jax.random.normal(shift_key, (C_OUT,), jnp.float32)
    return {"activations": activations, "conv_w": conv_w, "bn_scale": bn_scale, "bn_shift": bn_shift}


def reference(activations, conv_w, bn_scale, bn_shift):
    kernel = conv_w.astype(jnp.float32)
    live_rows = activations[:IMAGES].astype(jnp.float32)
    conv_blocks = live_rows.reshape(IMAGES // IMG_BLOCK, IMG_BLOCK, HEIGHT, WIDTH, C_IN)

    def one_block(x_block):
        pre_act = lax.conv_general_dilated(x_block, kernel, (1, 1), "SAME", dimension_numbers=CONV_DIMS)
        y_val = pre_act * bn_scale + bn_shift
        return jnp.maximum(y_val, 0.0).astype(jnp.bfloat16)

    z_rows = lax.map(one_block, conv_blocks).reshape(IMAGES, HEIGHT, WIDTH, C_OUT)
    return jnp.concatenate([jnp.zeros_like(z_rows), z_rows], axis=0)
```

```python
import functools

import jax
import jax.numpy as jnp
from jax import lax
from jax.experimental import pallas as pl
from jax.experimental.pallas import tpu as pltpu
from jax.sharding import PartitionSpec as P

MESH = pl.DeviceIdType.MESH
H, W, C = 28, 28, 256
N_LOC = 32
TP = 4
CB = C // TP
LANES = 128
PAIRS = W // 2
Q = 7
FLUSH = 14
VL = 46 * 2**20


def kernel(act, w, scale, shift, out, xpad, buf, wf, sb, xsem, wlsem, wssem, wrsem, bssem, brsem, ssem, rsem):
    pp, tp = lax.axis_index("pp"), lax.axis_index("tp")
    chip, core = tp // 2, tp % 2
    far = 1 - chip

    def w_copy(owner, part, half, slot, target):
        return pltpu.make_async_remote_copy(
            src_ref=w.at[:, :, pl.ds(pl.multiple_of(half * LANES, LANES), LANES)],
            dst_ref=wf.at[half, :, owner],
            send_sem=wssem.at[part, slot],
            recv_sem=wrsem.at[part, owner],
            device_id=target,
            device_id_type=MESH,
        )

    def w_local(half, part):
        return pltpu.make_async_copy(
            w.at[:, :, pl.ds(pl.multiple_of(half * LANES, LANES), LANES)], wf.at[half, :, tp], wlsem.at[part])

    def x_copy(h):
        return pltpu.make_async_copy(act.at[h], xpad.at[h + 1, pl.ds(1, W)], xsem.at[h])

    def b_copy(k, owner):
        return pltpu.make_async_remote_copy(
            src_ref=sb.at[tp], dst_ref=sb.at[tp], send_sem=bssem.at[k], recv_sem=brsem.at[owner],
            device_id=(0, lax.rem(tp + k, TP)), device_id_type=MESH)

    def z_copy(h, t, owner):
        return pltpu.make_async_remote_copy(
            src_ref=buf.at[h, :, t], dst_ref=buf.at[h, :, owner], send_sem=ssem.at[h, t], recv_sem=rsem.at[h, owner],
            device_id=(1, t), device_id_type=MESH)

    @pl.when(pp == 0)
    def _():
        for part in range(2):
            w_local(chip if part == 0 else far, part).start()

        def start_x(h, _):
            x_copy(h).start()
            return 0
        lax.fori_loop(0, H, start_x, 0)
        sb[tp, 0:1, :] = jnp.concatenate([scale[...], scale[...]], axis=1)
        sb[tp, 1:2, :] = jnp.concatenate([shift[...], shift[...]], axis=1)

    barrier = pltpu.get_barrier_semaphore()
    for d in range(1, 2 * TP):
        other = lax.rem(pp * TP + tp + d, 2 * TP)
        pl.semaphore_signal(barrier, inc=1, device_id=(other // TP, other % TP), device_id_type=MESH)
    pl.semaphore_wait(barrier, 2 * TP - 1)

    def far_sends(act_on):
        for part in range(2):
            half = far if part == 0 else chip
            for c in range(2):
                act_on(w_copy(tp, part, half, c, (0, far * 2 + c)))

    def near_sends(act_on):
        for part in range(2):
            half = chip if part == 0 else far
            act_on(w_copy(tp, part, half, 2, (0, chip * 2 + 1 - core)))

    sends_far = jnp.logical_or(jnp.logical_and(pp == 0, core == 0), jnp.logical_and(pp == 1, core == 1))

    @pl.when(sends_far)
    def _():
        far_sends(lambda c: c.start())

    @pl.when(pp == 0)
    def _():
        near_sends(lambda c: c.start())
        for k in range(1, TP):
            b_copy(k, tp).start()

        zero = jnp.zeros((W + 2, N_LOC, C), jnp.bfloat16)
        xpad[0] = zero
        xpad[H + 1] = zero
        xpad[:, 0] = zero
        xpad[:, W + 1] = zero

        for k in range(1, TP):
            b_copy(k, lax.rem(tp + k, TP)).wait_recv()

        lane = lax.broadcasted_iota(jnp.int32, (1, LANES), 1)
        low = lane < CB

        def wait_w(part, half):
            w_local(half, part).wait()
            for k in range(1, TP):
                owner = lax.rem(tp + k, TP)
                w_copy(owner, part, half, 0, (0, owner)).wait_recv()

        def step(h, half):
            sc = jnp.where(low, sb[2 * half, 0:1, :], sb[2 * half + 1, 0:1, :])
            sh = jnp.where(low, sb[2 * half, 1:2, :], sb[2 * half + 1, 1:2, :])

            def conv(w0):
                acc = None
                for a in range(3):
                    for b in range(3):
                        lhs = xpad[h + a, pl.ds(w0 + b, Q)].reshape(Q * N_LOC, C)
                        rhs = wf[half, 3 * a + b].reshape(C, LANES)
                        part = jnp.dot(lhs, rhs, preferred_element_type=jnp.float32)
                        acc = part if acc is None else acc + part
                return jnp.maximum(acc * sc + sh, 0.0)

            for q in range(PAIRS // Q):
                even, odd = conv(q * Q), conv(PAIRS + q * Q)
                first = jnp.where(low, even, pltpu.roll(odd, CB, 1)).astype(jnp.bfloat16)
                second = jnp.where(low, pltpu.roll(even, CB, 1), odd).astype(jnp.bfloat16)
                buf[h, pl.ds(q * Q, Q), 2 * half] = first.reshape(Q, N_LOC, LANES)
                buf[h, pl.ds(q * Q, Q), 2 * half + 1] = second.reshape(Q, N_LOC, LANES)
            for k in range(2):
                z_copy(h, 2 * half + k, tp).start()

        def row(h, _):
            @pl.when(h == 0)
            def _():
                x_copy(0).wait()

            @pl.when(h < H - 1)
            def _():
                x_copy(h + 1).wait()

            def both(j, _):
                half = jnp.where(j == 0, chip, far)

                @pl.when(h == 0)
                def _():
                    wait_w(j, half)
                step(h, half)
                return 0
            lax.fori_loop(0, 2, both, 0)
            return 0
        lax.fori_loop(0, H, row, 0)

        def clear(h, _):
            out[h] = jnp.zeros((W, CB, LANES), jnp.bfloat16)
            return 0
        lax.fori_loop(0, H, clear, 0)

        near_sends(lambda c: c.wait_send())
        for k in range(1, TP):
            b_copy(k, tp).wait_send()

        def drain(h, _):
            for t in range(TP):
                z_copy(h, t, tp).wait_send()
            return 0
        lax.fori_loop(0, H, drain, 0)

    @pl.when(sends_far)
    def _():
        far_sends(lambda c: c.wait_send())

    @pl.when(pp == 1)
    def _():
        def row(h, _):
            for s in range(TP):
                z_copy(h, s, s).wait_recv()

            def pair(p, _):
                block = buf[h, p].reshape(LANES, LANES)
                turned = block.T
                out[h, p] = turned[:CB]
                out[h, p + PAIRS] = turned[CB:]
                return 0
            lax.fori_loop(0, PAIRS, pair, 0)
            return 0
        lax.fori_loop(0, H, row, 0)


def flush(src, dst, sem):
    rows = H // FLUSH
    copies = [pltpu.make_async_copy(src.at[pl.ds(i * rows, rows)], dst.at[pl.ds(i * rows, rows)], sem.at[i])
              for i in range(FLUSH)]
    for c in copies:
        c.start()
    for c in copies:
        c.wait()


def solution(mesh):
    def local_step(act, w, scale, shift):
        x = jnp.transpose(act, (1, 2, 0, 3))
        dma = pltpu.SemaphoreType.DMA
        out = pl.pallas_call(
            kernel,
            out_shape=pltpu.VMEM((H, W, CB, LANES), jnp.bfloat16),
            in_specs=[pl.BlockSpec(memory_space=pl.ANY), pl.BlockSpec(memory_space=pl.ANY),
                      pl.BlockSpec(memory_space=pltpu.VMEM), pl.BlockSpec(memory_space=pltpu.VMEM)],
            out_specs=pl.BlockSpec(memory_space=pltpu.VMEM),
            scratch_shapes=[
                pltpu.VMEM((H + 2, W + 2, N_LOC, C), jnp.bfloat16),
                pltpu.VMEM((H, PAIRS, TP, N_LOC, LANES), jnp.bfloat16),
                pltpu.VMEM((2, 9, TP, C // TP, LANES), jnp.bfloat16),
                pltpu.VMEM((TP, 8, LANES), jnp.float32),
                dma((H,)), dma((2,)), dma((2, 3)), dma((2, TP)), dma((TP,)), dma((TP,)), dma((H, TP)), dma((H, TP)),
            ],
            compiler_params=pltpu.CompilerParams(collective_id=0, has_side_effects=True, vmem_limit_bytes=VL),
        )(x, w.reshape(9, C // TP, C), scale.reshape(1, CB), shift.reshape(1, CB))
        out = pl.pallas_call(
            flush,
            out_shape=jax.ShapeDtypeStruct((H, W, CB, LANES), jnp.bfloat16),
            in_specs=[pl.BlockSpec(memory_space=pltpu.VMEM)],
            out_specs=pl.BlockSpec(memory_space=pl.ANY),
            scratch_shapes=[dma((FLUSH,))],
            compiler_params=pltpu.CompilerParams(vmem_limit_bytes=2**20),
        )(out)
        return jnp.transpose(out, (3, 0, 1, 2))

    return jax.shard_map(local_step, mesh=mesh, in_specs=(P(("pp", "tp")), P(None, None, "tp", None), P("tp"), P("tp")),
                         out_specs=P("pp", None, None, "tp"), check_vma=False)
```

```python
import jax
import jax.numpy as jnp
from jax import lax
from jax.experimental import pallas as pl
from jax.experimental.pallas import tpu as pltpu
from jax.sharding import PartitionSpec as P

MESH = pl.DeviceIdType.MESH
H, W, C = 28, 28, 256
N_LOC = 32
TP = 4
CB = C // TP
LANES = 128
PAIRS = W // 2
Q = 7
G = 4
GROUPS = H // G
LAST = H - 1
FLUSH = 14
PARTS = ((0, 3, 6), (0, 0, 3), (1, 0, 9))


def kernel(act, w, scale, shift, out, xpad, buf, wf, sb, xsem, wlsem, wssem, wrsem, bssem, brsem, ssem, rsem, esem, fsem):
    pp, tp = lax.axis_index("pp"), lax.axis_index("tp")
    chip, core = tp // 2, tp % 2
    far = 1 - chip

    def half_of(sel, receiver):
        return receiver if sel == 0 else 1 - receiver

    def w_local(half):
        return pltpu.make_async_copy(
            w.at[:, :, pl.ds(pl.multiple_of(half * LANES, LANES), LANES)], wf.at[half, :, tp], wlsem.at[half])

    def w_copy(part, owner, slot, target):
        sel, tap, taps = PARTS[part]
        block = wf.at[half_of(sel, target // 2), pl.ds(tap, taps), owner]
        return pltpu.make_async_remote_copy(
            src_ref=block, dst_ref=block, send_sem=wssem.at[part, slot], recv_sem=wrsem.at[part, owner],
            device_id=(0, target), device_id_type=MESH)

    def x_copy(h):
        return pltpu.make_async_copy(act.at[h], xpad.at[h + 1, pl.ds(1, W)], xsem.at[h])

    def b_copy(k, owner):
        return pltpu.make_async_remote_copy(
            src_ref=sb.at[tp], dst_ref=sb.at[tp], send_sem=bssem.at[k], recv_sem=brsem.at[owner],
            device_id=(0, lax.rem(tp + k, TP)), device_id_type=MESH)

    def z_copy(h, rows, t, owner):
        return pltpu.make_async_remote_copy(
            src_ref=buf.at[pl.ds(h, rows), :, t], dst_ref=buf.at[pl.ds(h, rows), :, owner],
            send_sem=ssem.at[h, t], recv_sem=rsem.at[h, owner], device_id=(1, t), device_id_type=MESH)

    def z_part(i, q, t, owner):
        h = 0 if i == 0 else LAST
        return pltpu.make_async_remote_copy(
            src_ref=buf.at[h, pl.ds(q * Q, Q), t], dst_ref=buf.at[h, pl.ds(q * Q, Q), owner],
            send_sem=esem.at[i, q, t], recv_sem=fsem.at[i, q, owner], device_id=(1, t), device_id_type=MESH)

    sends_far = pp == core

    @pl.when(jnp.logical_or(pp == 0, sends_far))
    def _():
        w_local(0).start()
        w_local(1).start()

    @pl.when(pp == 0)
    def _():
        def start_x(h, _):
            x_copy(h).start()
            return 0
        lax.fori_loop(0, H, start_x, 0)
        sb[tp, 0:1, :] = jnp.concatenate([scale[...], scale[...]], axis=1)
        sb[tp, 1:2, :] = jnp.concatenate([shift[...], shift[...]], axis=1)

    barrier = pltpu.get_barrier_semaphore()
    for d in range(1, 2 * TP):
        other = lax.rem(pp * TP + tp + d, 2 * TP)
        pl.semaphore_signal(barrier, inc=1, device_id=(other // TP, other % TP), device_id_type=MESH)

    @pl.when(jnp.logical_or(pp == 0, sends_far))
    def _():
        w_local(0).wait()
        w_local(1).wait()
    pl.semaphore_wait(barrier, 2 * TP - 1)

    @pl.when(pp == 0)
    def _():
        for k in range(1, TP):
            b_copy(k, tp).start()

    def w_sends(act_on):
        for part in range(len(PARTS)):
            @pl.when(sends_far)
            def _():
                for c in range(2):
                    act_on(w_copy(part, tp, c, far * 2 + c))

            @pl.when(pp == 0)
            def _():
                act_on(w_copy(part, tp, 2, chip * 2 + 1 - core))

    w_sends(lambda c: c.start())

    @pl.when(pp == 0)
    def _():
        zero = jnp.zeros((W + 2, N_LOC, C), jnp.bfloat16)
        xpad[0] = zero
        xpad[H + 1] = zero
        xpad[:, 0] = zero
        xpad[:, W + 1] = zero

        for k in range(1, TP):
            b_copy(k, lax.rem(tp + k, TP)).wait_recv()

        low = lax.broadcasted_iota(jnp.int32, (1, LANES), 1) < CB

        def wait_w(part):
            for k in range(1, TP):
                w_copy(part, lax.rem(tp + k, TP), 0, tp).wait_recv()

        def pixels(h, half, q, first_tap):
            sc = jnp.where(low, sb[2 * half, 0:1, :], sb[2 * half + 1, 0:1, :])
            sh = jnp.where(low, sb[2 * half, 1:2, :], sb[2 * half + 1, 1:2, :])

            def conv(w0):
                acc = None
                for tap in range(first_tap, 9):
                    lhs = xpad[h + tap // 3, pl.ds(w0 + tap % 3, Q)].reshape(Q * N_LOC, C)
                    part = jnp.dot(lhs, wf[half, tap].reshape(C, LANES), preferred_element_type=jnp.float32)
                    acc = part if acc is None else acc + part
                return jnp.maximum(acc * sc + sh, 0.0)

            even, odd = conv(q * Q), conv(PAIRS + q * Q)
            first = jnp.where(low, even, pltpu.roll(odd, CB, 1)).astype(jnp.bfloat16)
            second = jnp.where(low, pltpu.roll(even, CB, 1), odd).astype(jnp.bfloat16)
            buf[h, pl.ds(q * Q, Q), 2 * half] = first.reshape(Q, N_LOC, LANES)
            buf[h, pl.ds(q * Q, Q), 2 * half + 1] = second.reshape(Q, N_LOC, LANES)

        x_copy(0).wait()
        x_copy(1).wait()
        wait_w(0)
        for q in range(2):
            pixels(0, chip, q, 3)
            for k in range(2):
                z_part(0, q, 2 * chip + k, tp).start()
        wait_w(1)

        def step(i, _):
            g, r = i // (2 * G), i % (2 * G)
            own = r < G
            half = jnp.where(own, chip, far)
            h = g * G + r % G

            @pl.when(i == G)
            def _():
                wait_w(2)

            @pl.when(jnp.logical_and(own, h < LAST))
            def _():
                x_copy(h + 1).wait()

            for q in range(2):
                pixels(h, half, q, 0)

                @pl.when(h == LAST)
                def _():
                    for k in range(2):
                        z_part(1, q, 2 * half + k, tp).start()

            edge = jnp.logical_or(g == 0, g == GROUPS - 1)

            @pl.when(jnp.logical_and(edge, jnp.logical_and(h < LAST, h > 0)))
            def _():
                for k in range(2):
                    z_copy(h, 1, 2 * half + k, tp).start()

            @pl.when(h == 0)
            def _():
                for q in range(2):
                    for k in range(2):
                        z_part(0, q, 2 * half + k, tp).start()

            @pl.when(jnp.logical_and(jnp.logical_not(edge), r % G == G - 1))
            def _():
                for k in range(2):
                    z_copy(g * G, G, 2 * half + k, tp).start()
            return 0
        lax.fori_loop(1, 2 * H, step, 0)

        def clear(h, _):
            out[h] = jnp.zeros((W, CB, LANES), jnp.bfloat16)
            return 0
        lax.fori_loop(0, H, clear, 0)

        for k in range(1, TP):
            b_copy(k, tp).wait_send()

    w_sends(lambda c: c.wait_send())

    @pl.when(pp == 0)
    def _():
        for t in range(TP):
            for i in range(2):
                for q in range(2):
                    z_part(i, q, t, tp).wait_send()
            for h in list(range(1, G)) + list(range(H - G, LAST)):
                z_copy(h, 1, t, tp).wait_send()

        def drain(g, _):
            for t in range(TP):
                z_copy(g * G, G, t, tp).wait_send()
            return 0
        lax.fori_loop(1, GROUPS - 1, drain, 0)

    @pl.when(pp == 1)
    def _():
        def turn(h, first, count):
            for p in range(first, first + count):
                turned = buf[h, p].reshape(LANES, LANES).T
                out[h, p] = turned[:CB]
                out[h, p + PAIRS] = turned[CB:]

        def group(g, _):
            edge = jnp.logical_or(g == 0, g == GROUPS - 1)

            @pl.when(jnp.logical_not(edge))
            def _():
                for s in range(TP):
                    z_copy(g * G, G, s, s).wait_recv()

            def row(h, _):
                @pl.when(jnp.logical_and(edge, jnp.logical_and(h < LAST, h > 0)))
                def _():
                    for s in range(TP):
                        z_copy(h, 1, s, s).wait_recv()
                for q in range(2):
                    for i in range(2):
                        @pl.when(h == i * LAST)
                        def _():
                            for s in range(TP):
                                z_part(i, q, s, s).wait_recv()
                    turn(h, q * Q, Q)
                return 0
            lax.fori_loop(g * G, g * G + G, row, 0)
            return 0
        lax.fori_loop(0, GROUPS, group, 0)


def flush(src, dst, sem):
    rows = H // FLUSH
    copies = [pltpu.make_async_copy(src.at[pl.ds(i * rows, rows)], dst.at[pl.ds(i * rows, rows)], sem.at[i])
              for i in range(FLUSH)]
    for c in copies:
        c.start()
    for c in copies:
        c.wait()


def solution(mesh):
    def local_step(act, w, scale, shift):
        x = jnp.transpose(act, (1, 2, 0, 3))
        dma = pltpu.SemaphoreType.DMA
        shape = (H, W, CB, LANES)
        out = pl.pallas_call(
            kernel,
            out_shape=pltpu.VMEM(shape, jnp.bfloat16),
            in_specs=[pl.BlockSpec(memory_space=pl.ANY), pl.BlockSpec(memory_space=pl.ANY),
                      pl.BlockSpec(memory_space=pltpu.VMEM), pl.BlockSpec(memory_space=pltpu.VMEM)],
            out_specs=pl.BlockSpec(memory_space=pltpu.VMEM),
            scratch_shapes=[
                pltpu.VMEM((H + 2, W + 2, N_LOC, C), jnp.bfloat16),
                pltpu.VMEM((H, PAIRS, TP, N_LOC, LANES), jnp.bfloat16),
                pltpu.VMEM((2, 9, TP, C // TP, LANES), jnp.bfloat16),
                pltpu.VMEM((TP, 8, LANES), jnp.float32),
                dma((H,)), dma((2,)), dma((3, 3)), dma((3, TP)), dma((TP,)), dma((TP,)), dma((H, TP)), dma((H, TP)),
                dma((2, 2, TP)), dma((2, 2, TP)),
            ],
            compiler_params=pltpu.CompilerParams(collective_id=0, has_side_effects=True, vmem_limit_bytes=46 * 2**20),
        )(x, w.reshape(9, C // TP, C), scale.reshape(1, CB), shift.reshape(1, CB))
        out = pl.pallas_call(
            flush,
            out_shape=jax.ShapeDtypeStruct(shape, jnp.bfloat16),
            in_specs=[pl.BlockSpec(memory_space=pltpu.VMEM)],
            out_specs=pl.BlockSpec(memory_space=pl.ANY),
            scratch_shapes=[dma((FLUSH,))],
            compiler_params=pltpu.CompilerParams(vmem_limit_bytes=2**20),
        )(out)
        return jnp.transpose(out, (3, 0, 1, 2))

    return jax.shard_map(local_step, mesh=mesh, in_specs=(P(("pp", "tp")), P(None, None, "tp", None), P("tp"), P("tp")),
                         out_specs=P("pp", None, None, "tp"), check_vma=False)
```

```python
import jax
import jax.numpy as jnp
from jax import lax
from jax.experimental import pallas as pl
from jax.experimental.pallas import tpu as pltpu
from jax.sharding import PartitionSpec as P

MESH = pl.DeviceIdType.MESH
H, W, C = 28, 28, 256
N_LOC = 32
TP = 4
CB = C // TP
LANES = 128
PAIRS = W // 2
Q = 7
G = 4
GROUPS = H // G
LAST = H - 1
FLUSH = 7
PARTS = ((0, 3, 6), (0, 0, 3), (1, 0, 9))
EDGES = ((1, 1), (2, 2), (H - 4, 2), (H - 2, 1))
EDGE_ROWS = 2
ENDS = (((0, 7), (7, 7)), ((0, 4), (4, 8), (12, 2)))


def kernel(act, w, scale, shift, out, xpad, buf, wf, sb, xsem, wlsem, wssem, wrsem, bssem, brsem, ssem, rsem, esem, fsem, vecs, vsem, ready):
    pp, tp = lax.axis_index("pp"), lax.axis_index("tp")
    chip, core = tp // 2, tp % 2
    far = 1 - chip

    def half_of(sel, receiver):
        return receiver if sel == 0 else 1 - receiver

    def w_local(half):
        return pltpu.make_async_copy(
            w.at[:, :, pl.ds(pl.multiple_of(half * LANES, LANES), LANES)], wf.at[half, :, tp], wlsem.at[half])

    def w_copy(part, owner, slot, target):
        sel, tap, taps = PARTS[part]
        block = wf.at[half_of(sel, target // 2), pl.ds(tap, taps), owner]
        return pltpu.make_async_remote_copy(
            src_ref=block, dst_ref=block, send_sem=wssem.at[part, slot], recv_sem=wrsem.at[part, owner],
            device_id=(0, target), device_id_type=MESH)

    def x_copy(h):
        return pltpu.make_async_copy(act.at[h], xpad.at[h + 1, pl.ds(1, W)], xsem.at[h])

    def vec_copy(i):
        return pltpu.make_async_copy((scale, shift)[i], vecs.at[i], vsem.at[i])

    def b_copy(k, owner):
        return pltpu.make_async_remote_copy(
            src_ref=sb.at[tp], dst_ref=sb.at[tp], send_sem=bssem.at[k], recv_sem=brsem.at[owner],
            device_id=(0, lax.rem(tp + k, TP)), device_id_type=MESH)

    def z_copy(h, rows, t, owner):
        return pltpu.make_async_remote_copy(
            src_ref=buf.at[pl.ds(h, rows), :, t], dst_ref=buf.at[pl.ds(h, rows), :, owner],
            send_sem=ssem.at[h, t], recv_sem=rsem.at[h, owner], device_id=(1, t), device_id_type=MESH)

    def z_part(i, q, t, owner):
        h = 0 if i == 0 else LAST
        return pltpu.make_async_remote_copy(
            src_ref=buf.at[h, pl.ds(*ENDS[i][q]), t], dst_ref=buf.at[h, pl.ds(*ENDS[i][q]), owner],
            send_sem=esem.at[i, q, t], recv_sem=fsem.at[i, q, owner], device_id=(1, t), device_id_type=MESH)

    def middle_done(t):
        def one(g, _):
            z_copy(g * G, G, t, tp).wait_send()
            return 0
        lax.fori_loop(1, GROUPS - 1, one, 0)

    barrier = pltpu.get_barrier_semaphore()

    @pl.when(pp == 0)
    def _():
        for k in range(1, TP):
            pl.semaphore_signal(barrier, inc=1, device_id=(0, lax.rem(tp + k, TP)), device_id_type=MESH)
        for k in range(TP):
            pl.semaphore_signal(barrier, inc=1, device_id=(1, lax.rem(tp + k, TP)), device_id_type=MESH)

    helps = jnp.logical_and(pp == 1, core == 1)
    has_w = jnp.logical_or(pp == 0, helps)

    @pl.when(pp == 0)
    def _():
        vec_copy(0).start()
        vec_copy(1).start()

    @pl.when(has_w)
    def _():
        w_local(0).start()
        w_local(1).start()

    @pl.when(pp == 0)
    def _():
        x_copy(0).start()
        x_copy(1).start()
        for i in range(2):
            vec_copy(i).wait()
            sb[tp, i : i + 1, :] = jnp.concatenate([vecs[i], vecs[i]], axis=1)

    pl.semaphore_wait(barrier, TP - 1 + pp)

    @pl.when(pp == 0)
    def _():
        for k in range(1, TP):
            b_copy(k, tp).start()

    @pl.when(has_w)
    def _():
        w_local(0).wait()
        w_local(1).wait()

    def w_sends(act_on):
        for part, cores in ((0, (0,)), (0, (1,)), (1, (0, 1)), (2, (0, 1))):
            near = part if cores[0] == 0 else None
            sends = jnp.logical_or(jnp.logical_and(pp == 0, core == 0), helps)
            if part == 0 and cores[0] == 0:
                sends = pp == 0

            @pl.when(sends)
            def _():
                for c in cores:
                    act_on(w_copy(part, tp, c, far * 2 + c))

            if near is not None:
                @pl.when(pp == 0)
                def _():
                    act_on(w_copy(near, tp, 2, chip * 2 + 1 - core))

    w_sends(lambda c: c.start())

    @pl.when(pp == 1)
    def _():
        for k in range(TP):
            pl.semaphore_signal(ready, inc=1, device_id=(0, lax.rem(tp + k, TP)), device_id_type=MESH)

    @pl.when(pp == 0)
    def _():
        def start_x(h, _):
            x_copy(h).start()
            return 0
        lax.fori_loop(2, H, start_x, 0)

        zero = jnp.zeros((W + 2, N_LOC, C), jnp.bfloat16)
        xpad[0] = zero
        xpad[H + 1] = zero
        xpad[:, 0] = zero
        xpad[:, W + 1] = zero

        for k in range(1, TP):
            b_copy(k, lax.rem(tp + k, TP)).wait_recv()

        low = lax.broadcasted_iota(jnp.int32, (1, LANES), 1) < CB

        def wait_w(part):
            for k in range(1, TP):
                w_copy(part, lax.rem(tp + k, TP), 0, tp).wait_recv()

        def pixels(h, half, q, first_tap):
            sc = jnp.where(low, sb[2 * half, 0:1, :], sb[2 * half + 1, 0:1, :])
            sh = jnp.where(low, sb[2 * half, 1:2, :], sb[2 * half + 1, 1:2, :])

            def conv(w0):
                acc = None
                for tap in range(first_tap, 9):
                    lhs = xpad[h + tap // 3, pl.ds(w0 + tap % 3, Q)].reshape(Q * N_LOC, C)
                    part = jnp.dot(lhs, wf[half, tap].reshape(C, LANES), preferred_element_type=jnp.float32)
                    acc = part if acc is None else acc + part
                return jnp.maximum(acc * sc + sh, 0.0)

            even, odd = conv(q * Q), conv(PAIRS + q * Q)
            first = jnp.where(low, even, pltpu.roll(odd, CB, 1)).astype(jnp.bfloat16)
            second = jnp.where(low, pltpu.roll(even, CB, 1), odd).astype(jnp.bfloat16)
            buf[h, pl.ds(q * Q, Q), 2 * half] = first.reshape(Q, N_LOC, LANES)
            buf[h, pl.ds(q * Q, Q), 2 * half + 1] = second.reshape(Q, N_LOC, LANES)

        x_copy(0).wait()
        x_copy(1).wait()
        wait_w(0)
        for q in range(2):
            pixels(0, chip, q, 3)
            if q == 0:
                pl.semaphore_wait(ready, TP)
            for k in range(2):
                z_part(0, q, 2 * chip + k, tp).start()
        wait_w(1)

        def last_sends(i, half, pieces):
            for q in pieces:
                for k in range(2):
                    z_part(i, q, 2 * half + k, tp).start()

        def step(i, _):
            g, r = i // (2 * G), i % (2 * G)
            own = r < G
            half = jnp.where(own, chip, far)
            h = g * G + r % G

            @pl.when(i == G)
            def _():
                wait_w(2)

            @pl.when(jnp.logical_and(own, h < LAST))
            def _():
                x_copy(h + 1).wait()

            for q in range(2):
                pixels(h, half, q, 0)

            @pl.when(h == 0)
            def _():
                last_sends(0, half, range(2))

            for first, rows in EDGES:
                @pl.when(h == first + rows - 1)
                def _():
                    for k in range(2):
                        z_copy(first, rows, 2 * half + k, tp).start()

            @pl.when(h == LAST)
            def _():
                last_sends(1, half, range(1))

            @pl.when(jnp.logical_and(h == LAST, jnp.logical_or(own, chip == 0)))
            def _():
                last_sends(1, half, range(1, 3))

            @pl.when(jnp.logical_and(jnp.logical_and(g > 0, g < GROUPS - 1), r % G == G - 1))
            def _():
                for k in range(2):
                    z_copy(g * G, G, 2 * half + k, tp).start()
            return 0
        lax.fori_loop(1, 2 * H, step, 0)

        def clear(h, _):
            out[h] = jnp.zeros((W, CB, LANES), jnp.bfloat16)
            return 0
        lax.fori_loop(0, H, clear, 0)

        @pl.when(chip == 1)
        def _():
            for k in range(2):
                z_copy(*EDGES[-1], 2 * chip + k, tp).wait_send()
            last_sends(1, far, range(1, 3))

        for k in range(1, TP):
            b_copy(k, tp).wait_send()

    w_sends(lambda c: c.wait_send())

    @pl.when(pp == 0)
    def _():
        for t in range(TP):
            for i in range(2):
                for q in range(len(ENDS[i])):
                    z_part(i, q, t, tp).wait_send()
            for first, rows in EDGES[:-1]:
                z_copy(first, rows, t, tp).wait_send()
            middle_done(t)
        for k in range(2):
            z_copy(*EDGES[-1], 2 * far + k, tp).wait_send()

        @pl.when(chip == 0)
        def _():
            for k in range(2):
                z_copy(*EDGES[-1], 2 * chip + k, tp).wait_send()

    @pl.when(pp == 1)
    def _():
        def turn(h, first, count):
            for p in range(first, first + count):
                turned = buf[h, p].reshape(LANES, LANES).T
                out[h, p] = turned[:CB]
                out[h, p + PAIRS] = turned[CB:]

        def arrived(first, rows):
            for s in range(TP):
                z_copy(first, rows, s, s).wait_recv()

        def turn_rows(first, rows):
            def row(h, _):
                turn(h, 0, PAIRS)
                return 0
            lax.fori_loop(first, first + rows, row, 0)

        def end(i):
            for q in range(len(ENDS[i])):
                for s in range(TP):
                    z_part(i, q, s, s).wait_recv()
                turn(i * LAST, *ENDS[i][q])

        end(0)
        for first, rows in EDGES[:EDGE_ROWS]:
            arrived(first, rows)
            turn_rows(first, rows)

        def group(g, _):
            arrived(g * G, G)
            turn_rows(g * G, G)
            return 0
        lax.fori_loop(1, GROUPS - 1, group, 0)
        for first, rows in EDGES[EDGE_ROWS:]:
            arrived(first, rows)
            turn_rows(first, rows)
        end(1)


def flush(src, dst, sem):
    rows = H // FLUSH
    copies = [pltpu.make_async_copy(src.at[pl.ds(i * rows, rows)], dst.at[pl.ds(i * rows, rows)], sem.at[i])
              for i in range(FLUSH)]
    for c in copies:
        c.start()
    for c in copies:
        c.wait()


def solution(mesh):
    def local_step(act, w, scale, shift):
        x = jnp.transpose(act, (1, 2, 0, 3))
        dma = pltpu.SemaphoreType.DMA
        shape = (H, W, CB, LANES)
        out = pl.pallas_call(
            kernel,
            out_shape=pltpu.VMEM(shape, jnp.bfloat16),
            in_specs=[pl.BlockSpec(memory_space=pl.ANY), pl.BlockSpec(memory_space=pl.ANY),
                      pl.BlockSpec(memory_space=pl.ANY), pl.BlockSpec(memory_space=pl.ANY)],
            out_specs=pl.BlockSpec(memory_space=pltpu.VMEM),
            scratch_shapes=[
                pltpu.VMEM((H + 2, W + 2, N_LOC, C), jnp.bfloat16),
                pltpu.VMEM((H, PAIRS, TP, N_LOC, LANES), jnp.bfloat16),
                pltpu.VMEM((2, 9, TP, C // TP, LANES), jnp.bfloat16),
                pltpu.VMEM((TP, 8, LANES), jnp.float32),
                dma((H,)), dma((2,)), dma((3, 3)), dma((3, TP)), dma((TP,)), dma((TP,)), dma((H, TP)), dma((H, TP)),
                dma((2, 3, TP)), dma((2, 3, TP)), pltpu.VMEM((2, 1, CB), jnp.float32), dma((2,)), pltpu.SemaphoreType.REGULAR,
            ],
            compiler_params=pltpu.CompilerParams(collective_id=0, has_side_effects=True, vmem_limit_bytes=46 * 2**20),
        )(x, w.reshape(9, C // TP, C), scale.reshape(1, CB), shift.reshape(1, CB))
        out = pl.pallas_call(
            flush,
            out_shape=jax.ShapeDtypeStruct(shape, jnp.bfloat16),
            in_specs=[pl.BlockSpec(memory_space=pltpu.VMEM)],
            out_specs=pl.BlockSpec(memory_space=pl.ANY),
            scratch_shapes=[dma((FLUSH,))],
            compiler_params=pltpu.CompilerParams(vmem_limit_bytes=2**20),
        )(out)
        return jnp.transpose(out, (3, 0, 1, 2))

    return jax.shard_map(local_step, mesh=mesh, in_specs=(P(("pp", "tp")), P(None, None, "tp", None), P("tp"), P("tp")),
                         out_specs=P("pp", None, None, "tp"), check_vma=False)
```

```python
import jax
import jax.numpy as jnp
from jax import lax
from jax.experimental import pallas as pl
from jax.experimental.pallas import tpu as pltpu
from jax.sharding import PartitionSpec as P

MESH = pl.DeviceIdType.MESH
H, W, C = 28, 28, 256
N_LOC = 32
TP = 4
CB = C // TP
LANES = 128
PAIRS = W // 2
Q = 7
G = 4
GROUPS = H // G
LAST = H - 1
FLUSH = 7
PARTS = ((0, 3, 3), (0, 6, 3), (0, 0, 3), (1, 0, 9))
ORDER = (1, 0)
EDGES = ((1, 1), (2, 2), (H - 4, 2), (H - 2, 1))
EDGE_ROWS = 2
FIRST = ((0, 0), (1, 0), (0, 1), (1, 1))
REST = ((2, 0), (2, 1), (3, 0), (3, 1))
ENDS = (((0, 7), (7, 7)), ((0, 4), (4, 8), (12, 2)))


def kernel(act, w, scale, shift, out, xpad, buf, wf, sb, xsem, wlsem, wssem, wrsem, bssem, brsem, ssem, rsem, esem, fsem, vecs, vsem, ready):
    pp, tp = lax.axis_index("pp"), lax.axis_index("tp")
    chip, core = tp // 2, tp % 2
    far = 1 - chip

    def half_of(sel, receiver):
        return receiver if sel == 0 else 1 - receiver

    def w_local(half):
        return pltpu.make_async_copy(
            w.at[:, :, pl.ds(pl.multiple_of(half * LANES, LANES), LANES)], wf.at[half, :, tp], wlsem.at[half])

    def w_copy(part, owner, slot, target):
        sel, tap, taps = PARTS[part]
        block = wf.at[half_of(sel, target // 2), pl.ds(tap, taps), owner]
        return pltpu.make_async_remote_copy(
            src_ref=block, dst_ref=block, send_sem=wssem.at[part, slot], recv_sem=wrsem.at[part, owner],
            device_id=(0, target), device_id_type=MESH)

    def x_copy(h):
        return pltpu.make_async_copy(act.at[h], xpad.at[h + 1, pl.ds(1, W)], xsem.at[h])

    def vec_copy(i):
        return pltpu.make_async_copy((scale, shift)[i], vecs.at[i], vsem.at[i])

    def b_copy(k, owner):
        return pltpu.make_async_remote_copy(
            src_ref=sb.at[tp], dst_ref=sb.at[tp], send_sem=bssem.at[k], recv_sem=brsem.at[owner],
            device_id=(0, lax.rem(tp + k, TP)), device_id_type=MESH)

    def z_copy(h, rows, t, owner):
        return pltpu.make_async_remote_copy(
            src_ref=buf.at[pl.ds(h, rows), :, t], dst_ref=buf.at[pl.ds(h, rows), :, owner],
            send_sem=ssem.at[h, t], recv_sem=rsem.at[h, owner], device_id=(1, t), device_id_type=MESH)

    def z_part(i, q, t, owner):
        h = 0 if i == 0 else LAST
        return pltpu.make_async_remote_copy(
            src_ref=buf.at[h, pl.ds(*ENDS[i][q]), t], dst_ref=buf.at[h, pl.ds(*ENDS[i][q]), owner],
            send_sem=esem.at[i, q, t], recv_sem=fsem.at[i, q, owner], device_id=(1, t), device_id_type=MESH)

    def middle_done(t):
        def one(g, _):
            z_copy(g * G, G, t, tp).wait_send()
            return 0
        lax.fori_loop(1, GROUPS - 1, one, 0)

    barrier = pltpu.get_barrier_semaphore()

    @pl.when(pp == 0)
    def _():
        for k in range(1, TP):
            pl.semaphore_signal(barrier, inc=1, device_id=(0, lax.rem(tp + k, TP)), device_id_type=MESH)
        for k in range(TP):
            pl.semaphore_signal(barrier, inc=1, device_id=(1, lax.rem(tp + k, TP)), device_id_type=MESH)

    helps = jnp.logical_and(pp == 1, core == 1)
    has_w = jnp.logical_or(pp == 0, helps)

    @pl.when(pp == 0)
    def _():
        vec_copy(0).start()
        vec_copy(1).start()

    @pl.when(has_w)
    def _():
        w_local(0).start()
        w_local(1).start()

    @pl.when(pp == 0)
    def _():
        x_copy(0).start()
        x_copy(1).start()
        for i in range(2):
            vec_copy(i).wait()
            sb[tp, i : i + 1, :] = jnp.concatenate([vecs[i], vecs[i]], axis=1)

    pl.semaphore_wait(barrier, TP - 1 + pp)

    @pl.when(pp == 1)
    def _():
        for k in range(TP):
            pl.semaphore_signal(ready, inc=1, device_id=(0, lax.rem(tp + k, TP)), device_id_type=MESH)

    @pl.when(pp == 0)
    def _():
        for k in range(1, TP):
            b_copy(k, tp).start()

    @pl.when(has_w)
    def _():
        w_local(0).wait()
        w_local(1).wait()

    def w_sends(act_on, stages):
        for part, c in stages:
            sends = jnp.logical_or(jnp.logical_and(pp == 0, core == 0), helps)
            if (part, c) == FIRST[0]:
                sends = pp == 0

            @pl.when(sends)
            def _():
                act_on(w_copy(part, tp, c, far * 2 + c))

            if c == 0:
                @pl.when(pp == 0)
                def _():
                    act_on(w_copy(part, tp, 2, chip * 2 + 1 - core))

    w_sends(lambda c: c.start(), FIRST)

    @pl.when(pp == 1)
    def _():
        w_sends(lambda c: c.start(), REST)

    @pl.when(pp == 0)
    def _():
        def start_x(h, _):
            x_copy(h).start()
            return 0
        lax.fori_loop(2, H, start_x, 0)

        zero = jnp.zeros((W + 2, N_LOC, C), jnp.bfloat16)
        xpad[0] = zero
        xpad[H + 1] = zero
        xpad[:, 0] = zero
        xpad[:, W + 1] = zero

        for k in range(1, TP):
            b_copy(k, lax.rem(tp + k, TP)).wait_recv()

        low = lax.broadcasted_iota(jnp.int32, (1, LANES), 1) < CB

        def wait_w(part):
            for k in range(1, TP):
                w_copy(part, lax.rem(tp + k, TP), 0, tp).wait_recv()

        def pixels(h, half, start, count, first_tap):
            sc = jnp.where(low, sb[2 * half, 0:1, :], sb[2 * half + 1, 0:1, :])
            sh = jnp.where(low, sb[2 * half, 1:2, :], sb[2 * half + 1, 1:2, :])

            def conv(w0):
                acc = None
                for tap in range(first_tap, 9):
                    lhs = xpad[h + tap // 3, pl.ds(w0 + tap % 3, count)].reshape(count * N_LOC, C)
                    part = jnp.dot(lhs, wf[half, tap].reshape(C, LANES), preferred_element_type=jnp.float32)
                    acc = part if acc is None else acc + part
                return jnp.maximum(acc * sc + sh, 0.0)

            even, odd = conv(start), conv(PAIRS + start)
            first = jnp.where(low, even, pltpu.roll(odd, CB, 1)).astype(jnp.bfloat16)
            second = jnp.where(low, pltpu.roll(even, CB, 1), odd).astype(jnp.bfloat16)
            buf[h, pl.ds(start, count), 2 * half] = first.reshape(count, N_LOC, LANES)
            buf[h, pl.ds(start, count), 2 * half + 1] = second.reshape(count, N_LOC, LANES)

        x_copy(0).wait()
        x_copy(1).wait()
        wait_w(0)
        wait_w(1)
        for q, (start, count) in enumerate(ENDS[0]):
            pixels(0, chip, start, count, 3)
            if q == 0:
                pl.semaphore_wait(ready, TP)
            for k in ORDER:
                z_part(0, q, 2 * chip + k, tp).start()
        w_sends(lambda c: c.start(), REST)
        wait_w(2)

        def last_sends(half, pieces):
            for q in pieces:
                for k in ORDER:
                    z_part(1, q, 2 * half + k, tp).start()

        def step(i, _):
            g, r = i // (2 * G), i % (2 * G)
            own = r < G
            half = jnp.where(own, chip, far)
            h = g * G + r % G

            @pl.when(i == G)
            def _():
                wait_w(3)

            @pl.when(jnp.logical_and(own, h < LAST))
            def _():
                x_copy(h + 1).wait()

            for q in range(2):
                pixels(h, half, q * Q, Q, 0)

            @pl.when(h == 0)
            def _():
                for k in ORDER:
                    z_copy(0, 1, 2 * half + k, tp).start()

            for first, rows in EDGES:
                @pl.when(h == first + rows - 1)
                def _():
                    for k in ORDER:
                        z_copy(first, rows, 2 * half + k, tp).start()

            @pl.when(h == LAST)
            def _():
                last_sends(half, range(1))

            @pl.when(jnp.logical_and(h == LAST, jnp.logical_or(own, chip == 0)))
            def _():
                last_sends(half, range(1, 3))

            @pl.when(jnp.logical_and(jnp.logical_and(g > 0, g < GROUPS - 1), r % G == G - 1))
            def _():
                for k in ORDER:
                    z_copy(g * G, G, 2 * half + k, tp).start()
            return 0
        lax.fori_loop(1, 2 * H, step, 0)

        def clear(h, _):
            out[h] = jnp.zeros((W, CB, LANES), jnp.bfloat16)
            return 0
        lax.fori_loop(0, H, clear, 0)

        @pl.when(chip == 1)
        def _():
            for k in range(2):
                z_copy(*EDGES[-1], 2 * chip + k, tp).wait_send()
            last_sends(far, range(1, 3))

        for k in range(1, TP):
            b_copy(k, tp).wait_send()

    w_sends(lambda c: c.wait_send(), FIRST + REST)

    @pl.when(pp == 0)
    def _():
        for t in range(TP):
            for q in range(len(ENDS[1])):
                z_part(1, q, t, tp).wait_send()
            for first, rows in EDGES[:-1]:
                z_copy(first, rows, t, tp).wait_send()
            middle_done(t)
        for k in range(2):
            for q in range(len(ENDS[0])):
                z_part(0, q, 2 * chip + k, tp).wait_send()
            z_copy(0, 1, 2 * far + k, tp).wait_send()
            z_copy(*EDGES[-1], 2 * far + k, tp).wait_send()

        @pl.when(chip == 0)
        def _():
            for k in range(2):
                z_copy(*EDGES[-1], 2 * chip + k, tp).wait_send()

    @pl.when(pp == 1)
    def _():
        def turn(h, first, count):
            for p in range(first, first + count):
                turned = buf[h, p].reshape(LANES, LANES).T
                out[h, p] = turned[:CB]
                out[h, p + PAIRS] = turned[CB:]

        def arrived(first, rows):
            for s in range(TP):
                z_copy(first, rows, s, s).wait_recv()

        def turn_rows(first, rows):
            def row(h, _):
                turn(h, 0, PAIRS)
                return 0
            lax.fori_loop(first, first + rows, row, 0)

        for k in range(2):
            for q in range(len(ENDS[0])):
                z_part(0, q, 2 * chip + k, 2 * chip + k).wait_recv()
            z_copy(0, 1, 2 * far + k, 2 * far + k).wait_recv()
        turn(0, 0, PAIRS)
        for first, rows in EDGES[:EDGE_ROWS]:
            arrived(first, rows)
            turn_rows(first, rows)

        def group(g, _):
            arrived(g * G, G)
            turn_rows(g * G, G)
            return 0
        lax.fori_loop(1, GROUPS - 1, group, 0)
        for first, rows in EDGES[EDGE_ROWS:]:
            arrived(first, rows)
            turn_rows(first, rows)
        for q in range(len(ENDS[1])):
            for s in range(TP):
                z_part(1, q, s, s).wait_recv()
            turn(LAST, *ENDS[1][q])


def flush(src, dst, sem):
    rows = H // FLUSH
    copies = [pltpu.make_async_copy(src.at[pl.ds(i * rows, rows)], dst.at[pl.ds(i * rows, rows)], sem.at[i])
              for i in range(FLUSH)]
    for c in copies:
        c.start()
    for c in copies:
        c.wait()


def solution(mesh):
    def local_step(act, w, scale, shift):
        x = jnp.transpose(act, (1, 2, 0, 3))
        dma = pltpu.SemaphoreType.DMA
        shape = (H, W, CB, LANES)
        out = pl.pallas_call(
            kernel,
            out_shape=pltpu.VMEM(shape, jnp.bfloat16),
            in_specs=[pl.BlockSpec(memory_space=pl.ANY), pl.BlockSpec(memory_space=pl.ANY),
                      pl.BlockSpec(memory_space=pl.ANY), pl.BlockSpec(memory_space=pl.ANY)],
            out_specs=pl.BlockSpec(memory_space=pltpu.VMEM),
            scratch_shapes=[
                pltpu.VMEM((H + 2, W + 2, N_LOC, C), jnp.bfloat16),
                pltpu.VMEM((H, PAIRS, TP, N_LOC, LANES), jnp.bfloat16),
                pltpu.VMEM((2, 9, TP, C // TP, LANES), jnp.bfloat16),
                pltpu.VMEM((TP, 8, LANES), jnp.float32),
                dma((H,)), dma((2,)), dma((4, 3)), dma((4, TP)), dma((TP,)), dma((TP,)), dma((H, TP)), dma((H, TP)),
                dma((2, 3, TP)), dma((2, 3, TP)), pltpu.VMEM((2, 1, CB), jnp.float32), dma((2,)), pltpu.SemaphoreType.REGULAR,
            ],
            compiler_params=pltpu.CompilerParams(collective_id=0, has_side_effects=True, vmem_limit_bytes=46 * 2**20),
        )(x, w.reshape(9, C // TP, C), scale.reshape(1, CB), shift.reshape(1, CB))
        out = pl.pallas_call(
            flush,
            out_shape=jax.ShapeDtypeStruct(shape, jnp.bfloat16),
            in_specs=[pl.BlockSpec(memory_space=pltpu.VMEM)],
            out_specs=pl.BlockSpec(memory_space=pl.ANY),
            scratch_shapes=[dma((FLUSH,))],
            compiler_params=pltpu.CompilerParams(vmem_limit_bytes=2**20),
        )(out)
        return jnp.transpose(out, (3, 0, 1, 2))

    return jax.shard_map(local_step, mesh=mesh, in_specs=(P(("pp", "tp")), P(None, None, "tp", None), P("tp"), P("tp")),
                         out_specs=P("pp", None, None, "tp"), check_vma=False)
```

```python
import functools

import jax
import jax.numpy as jnp
from jax import lax
from jax.experimental import pallas as pl
from jax.experimental.pallas import tpu as pltpu
from jax.sharding import PartitionSpec as P

MESH = pl.DeviceIdType.MESH
H, W, C = 28, 28, 256
N_LOC = 32
TP = 4
CB = C // TP
LANES = 128
PAIRS = W // 2
Q = 7
G = 4
GROUPS = H // G
LAST = H - 1
SPLIT = 20
ODD_SPLIT = 24
LATE = H - SPLIT
PARTS = ((0, 3, 3), (0, 6, 3), (0, 0, 3), (1, 0, 9))
ORDER = (1, 0)
FIRST = ((0, 0), (1, 0), (0, 1), (1, 1))
REST = ((2, 0), (2, 1), (3, 0), (3, 1))
HEAD = ((0, 7), (7, 7))
ROWS = ((1, 1), (2, 2), (4, 4), (8, 8), (16, 4))
ODD_ROWS = (SPLIT, ODD_SPLIT - SPLIT)
LATE_EVEN = ((0, 4), (4, 2), (6, 1))
LATE_ODD = ((4, 2), (6, 1))
TAIL = ((0, 7), (7, 5), (12, 2))


def kernel(act, w, scale, shift, out, buf, xpad, wf, sb, xsem, wlsem, wssem, wrsem, bssem, brsem, ssem, rsem, esem, fsem, vecs, vsem, ready):
    pp, tp = lax.axis_index("pp"), lax.axis_index("tp")
    chip, core = tp // 2, tp % 2
    far = 1 - chip

    def half_of(sel, receiver):
        return receiver if sel == 0 else 1 - receiver

    def w_local(half):
        return pltpu.make_async_copy(
            w.at[:, :, pl.ds(pl.multiple_of(half * LANES, LANES), LANES)], wf.at[half, :, tp], wlsem.at[half])

    def w_copy(part, owner, slot, target):
        sel, tap, taps = PARTS[part]
        block = wf.at[half_of(sel, target // 2), pl.ds(tap, taps), owner]
        return pltpu.make_async_remote_copy(
            src_ref=block, dst_ref=block, send_sem=wssem.at[part, slot], recv_sem=wrsem.at[part, owner],
            device_id=(0, target), device_id_type=MESH)

    def x_copy(h):
        return pltpu.make_async_copy(act.at[h], xpad.at[h + 1, pl.ds(1, W)], xsem.at[h])

    def vec_copy(i):
        return pltpu.make_async_copy((scale, shift)[i], vecs.at[i], vsem.at[i])

    def b_copy(k, owner):
        return pltpu.make_async_remote_copy(
            src_ref=sb.at[tp], dst_ref=sb.at[tp], send_sem=bssem.at[k], recv_sem=brsem.at[owner],
            device_id=(0, lax.rem(tp + k, TP)), device_id_type=MESH)

    def z_copy(h, rows, t, owner):
        return pltpu.make_async_remote_copy(
            src_ref=buf.at[pl.ds(h, rows), :, t], dst_ref=buf.at[pl.ds(h, rows), :, owner],
            send_sem=ssem.at[h, t], recv_sem=rsem.at[h, owner], device_id=(1, t), device_id_type=MESH)

    def z_head(q, t, owner):
        return pltpu.make_async_remote_copy(
            src_ref=buf.at[0, pl.ds(*HEAD[q]), t], dst_ref=buf.at[0, pl.ds(*HEAD[q]), owner],
            send_sem=esem.at[q, t], recv_sem=fsem.at[q, owner], device_id=(1, t), device_id_type=MESH)

    barrier = pltpu.get_barrier_semaphore()

    @pl.when(pp == 0)
    def _():
        for k in range(1, TP):
            pl.semaphore_signal(barrier, inc=1, device_id=(0, lax.rem(tp + k, TP)), device_id_type=MESH)
        for k in range(TP):
            pl.semaphore_signal(barrier, inc=1, device_id=(1, lax.rem(tp + k, TP)), device_id_type=MESH)

    helps = jnp.logical_and(pp == 1, core == 1)
    has_w = jnp.logical_or(pp == 0, helps)

    @pl.when(pp == 0)
    def _():
        vec_copy(0).start()
        vec_copy(1).start()

    @pl.when(has_w)
    def _():
        w_local(0).start()
        w_local(1).start()

    @pl.when(pp == 0)
    def _():
        x_copy(0).start()
        x_copy(1).start()
        for i in range(2):
            vec_copy(i).wait()
            sb[tp, i : i + 1, :] = jnp.concatenate([vecs[i], vecs[i]], axis=1)

    pl.semaphore_wait(barrier, TP - 1 + pp)

    @pl.when(pp == 1)
    def _():
        for k in range(TP):
            pl.semaphore_signal(ready, inc=1, device_id=(0, lax.rem(tp + k, TP)), device_id_type=MESH)

    @pl.when(pp == 0)
    def _():
        for k in range(1, TP):
            b_copy(k, tp).start()

    @pl.when(has_w)
    def _():
        w_local(0).wait()
        w_local(1).wait()

    def w_sends(act_on, stages):
        for part, c in stages:
            sends = jnp.logical_or(jnp.logical_and(pp == 0, core == 0), helps)
            if (part, c) == FIRST[0]:
                sends = pp == 0

            @pl.when(sends)
            def _():
                act_on(w_copy(part, tp, c, far * 2 + c))

            if c == 0:
                @pl.when(pp == 0)
                def _():
                    act_on(w_copy(part, tp, 2, chip * 2 + 1 - core))

    w_sends(lambda c: c.start(), FIRST)

    @pl.when(pp == 1)
    def _():
        w_sends(lambda c: c.start(), REST)

    @pl.when(pp == 0)
    def _():
        def start_x(h, _):
            x_copy(h).start()
            return 0
        lax.fori_loop(2, H, start_x, 0)

        zero = jnp.zeros((W + 2, N_LOC, C), jnp.bfloat16)
        xpad[0] = zero
        xpad[H + 1] = zero
        xpad[:, 0] = zero
        xpad[:, W + 1] = zero

        for k in range(1, TP):
            b_copy(k, lax.rem(tp + k, TP)).wait_recv()

        low = lax.broadcasted_iota(jnp.int32, (1, LANES), 1) < CB

        def wait_w(part):
            for k in range(1, TP):
                w_copy(part, lax.rem(tp + k, TP), 0, tp).wait_recv()

        def pixels(h, half, start, count, first_tap):
            sc = jnp.where(low, sb[2 * half, 0:1, :], sb[2 * half + 1, 0:1, :])
            sh = jnp.where(low, sb[2 * half, 1:2, :], sb[2 * half + 1, 1:2, :])

            def conv(w0):
                acc = None
                for tap in range(first_tap, 9):
                    lhs = xpad[h + tap // 3, pl.ds(w0 + tap % 3, count)].reshape(count * N_LOC, C)
                    part = jnp.dot(lhs, wf[half, tap].reshape(C, LANES), preferred_element_type=jnp.float32)
                    acc = part if acc is None else acc + part
                return jnp.maximum(acc * sc + sh, 0.0)

            even, odd = conv(start), conv(PAIRS + start)
            first = jnp.where(low, even, pltpu.roll(odd, CB, 1)).astype(jnp.bfloat16)
            second = jnp.where(low, pltpu.roll(even, CB, 1), odd).astype(jnp.bfloat16)
            buf[h, pl.ds(start, count), 2 * half] = first.reshape(count, N_LOC, LANES)
            buf[h, pl.ds(start, count), 2 * half + 1] = second.reshape(count, N_LOC, LANES)

        x_copy(0).wait()
        x_copy(1).wait()
        wait_w(0)
        wait_w(1)
        for q, (start, count) in enumerate(HEAD):
            pixels(0, chip, start, count, 3)
            if q == 0:
                pl.semaphore_wait(ready, TP)
            for k in ORDER:
                z_head(q, 2 * chip + k, tp).start()
        w_sends(lambda c: c.start(), REST)
        wait_w(2)

        def step(i, _):
            g, r = i // (2 * G), i % (2 * G)
            own = r < G
            half = jnp.where(own, chip, far)
            h = g * G + r % G

            @pl.when(i == G)
            def _():
                wait_w(3)

            @pl.when(jnp.logical_and(own, h < LAST))
            def _():
                x_copy(h + 1).wait()

            for q in range(2):
                pixels(h, half, q * Q, Q, 0)

            def send(first, rows, cores):
                for k in cores:
                    z_copy(first, rows, 2 * half + k, tp).start()

            @pl.when(h == 0)
            def _():
                send(0, 1, (0, 1))

            for first, rows in ROWS[:-1]:
                @pl.when(h == first + rows - 1)
                def _():
                    send(first, rows, (0, 1))

            last = jnp.logical_and(own, core == 1)

            @pl.when(h == SPLIT - 1)
            def _():
                send(*ROWS[-1], (0,))

            @pl.when(jnp.logical_and(h == SPLIT - 1, jnp.logical_not(last)))
            def _():
                send(*ROWS[-1], (1,))

            @pl.when(jnp.logical_and(h == ODD_SPLIT - 1, core == 1))
            def _():
                send(*ODD_ROWS, (0,))

            @pl.when(jnp.logical_and(h == ODD_SPLIT - 1, last))
            def _():
                send(*ROWS[-1], (1,))

            @pl.when(jnp.logical_and(h == ODD_SPLIT - 1, core == 1))
            def _():
                send(*ODD_ROWS, (1,))
            return 0
        lax.fori_loop(1, 2 * H, step, 0)

        def clear(h, _):
            out[h] = jnp.zeros((W, CB, LANES), jnp.bfloat16)
            return 0
        lax.fori_loop(0, SPLIT, clear, 0)

        for k in range(1, TP):
            b_copy(k, tp).wait_send()

    w_sends(lambda c: c.wait_send(), FIRST + REST)

    @pl.when(pp == 0)
    def _():
        for k in range(2):
            for q in range(len(HEAD)):
                z_head(q, 2 * chip + k, tp).wait_send()
            z_copy(0, 1, 2 * far + k, tp).wait_send()
        for t in range(TP):
            for first, rows in ROWS:
                z_copy(first, rows, t, tp).wait_send()

            @pl.when(core == 1)
            def _():
                z_copy(*ODD_ROWS, t, tp).wait_send()

    @pl.when(pp == 1)
    def _():
        def turn_rows(first, rows):
            def row(h, _):
                for p in range(PAIRS):
                    turn(buf[h, p].reshape(LANES, LANES), out, h, p)
                return 0
            lax.fori_loop(first, first + rows, row, 0)

        for k in range(2):
            for q in range(len(HEAD)):
                z_head(q, 2 * chip + k, 2 * chip + k).wait_recv()
            z_copy(0, 1, 2 * far + k, 2 * far + k).wait_recv()
        turn_rows(0, 1)
        for first, rows in ROWS:
            for s in range(TP):
                z_copy(first, rows, s, s).wait_recv()
            turn_rows(first, rows)
        for s in (1, 3):
            z_copy(*ODD_ROWS, s, s).wait_recv()


def turn(block, out, h, p):
    turned = block.T
    out[h, p] = turned[:CB]
    out[h, p + PAIRS] = turned[CB:]


def finish(z, _, out, got, ssem, rsem, tsem, usem, ready):
    pp, tp = lax.axis_index("pp"), lax.axis_index("tp")
    core = tp % 2
    source = pp == 0
    even = core == 0

    def z_copy(first, rows, t, owner):
        return pltpu.make_async_remote_copy(
            src_ref=z.at[pl.ds(SPLIT + first, rows), :, t], dst_ref=got.at[pl.ds(first, rows), :, owner],
            send_sem=ssem.at[first, t], recv_sem=rsem.at[first, owner], device_id=(1, t), device_id_type=MESH)

    def z_tail(q, t, owner):
        return pltpu.make_async_remote_copy(
            src_ref=z.at[LAST, pl.ds(*TAIL[q]), t], dst_ref=got.at[LATE - 1, pl.ds(*TAIL[q]), owner],
            send_sem=tsem.at[q, t], recv_sem=usem.at[q, owner], device_id=(1, t), device_id_type=MESH)

    def copies(rows, t, owner):
        return [z_copy(*r, t, owner) for r in rows] + [z_tail(q, t, owner) for q in range(len(TAIL))]

    barrier = pltpu.get_barrier_semaphore()

    def greet(where, targets):
        @pl.when(where)
        def _():
            for target in targets:
                pl.semaphore_signal(barrier, inc=1, device_id=target, device_id_type=MESH)

    greet(source & even, [(1, 0), (1, 2), (1, 1), (1, 3), (0, lax.rem(tp + 2, TP))])
    greet(source & ~even, [(1, 1), (1, 3)])
    greet(~source & even, [(0, 1), (0, 3)])
    pl.semaphore_wait(barrier, jnp.where(source, jnp.where(even, 1, 2), jnp.where(even, 2, 4)))

    @pl.when(~source & even)
    def _():
        for t in (0, 2):
            pl.semaphore_signal(ready.at[0], inc=1, device_id=(0, t), device_id_type=MESH)

    @pl.when(~source & ~even)
    def _():
        for t in range(TP):
            pl.semaphore_signal(ready.at[1], inc=1, device_id=(0, t), device_id_type=MESH)

    def sends(rows, k):
        for a in zip(*[copies(rows, t, tp) for t in (k, 2 + k)]):
            for c in a:
                c.start()

    @pl.when(source & even)
    def _():
        pl.semaphore_wait(ready.at[0], 2)
        sends(LATE_EVEN, 0)
        pl.semaphore_wait(ready.at[1], 2)
        sends(LATE_EVEN, 1)

    @pl.when(source & ~even)
    def _():
        sends(LATE_ODD, 0)
        pl.semaphore_wait(ready.at[1], 2)
        sends(LATE_ODD, 1)

    @pl.when(source)
    def _():
        def clear(h, _):
            out[h] = jnp.zeros((W, CB, LANES), jnp.bfloat16)
            return 0
        lax.fori_loop(0, LATE, clear, 0)
        for rows, where in ((LATE_EVEN, even), (LATE_ODD, ~even)):
            @pl.when(where)
            def _():
                for t in range(TP):
                    for c in copies(rows, t, tp):
                        c.wait_send()

    @pl.when(~source)
    def _():
        for s in (0, 2):
            z_copy(*LATE_EVEN[0], s, s).wait_recv()

        def mixed(h, _):
            for p in range(PAIRS):
                parts = [got[h, p, s] if s % 2 == 0 else z[SPLIT + h, p, s] for s in range(TP)]
                turn(jnp.concatenate(parts, axis=0), out, h, p)
            return 0
        lax.fori_loop(0, ODD_SPLIT - SPLIT, mixed, 0)
        for first, rows in LATE_ODD:
            for s in range(TP):
                z_copy(first, rows, s, s).wait_recv()

            def row(h, _):
                for p in range(PAIRS):
                    turn(got[h, p].reshape(LANES, LANES), out, h, p)
                return 0
            lax.fori_loop(first, first + rows, row, 0)
        for q, (start, count) in enumerate(TAIL):
            for s in range(TP):
                z_tail(q, s, s).wait_recv()
            for p in range(start, start + count):
                turn(got[LATE - 1, p].reshape(LANES, LANES), out, LATE - 1, p)


def write(first, rows, each, src, *refs):
    dst, _, sem = refs[-3:]
    copies = [pltpu.make_async_copy(src.at[pl.ds(i * each, each)], dst.at[pl.ds(first + i * each, each)], sem.at[i])
              for i in range(rows // each)]
    for c in copies:
        c.start()
    for c in copies:
        c.wait()


def solution(mesh):
    def local_step(act, w, scale, shift):
        x = jnp.transpose(act, (1, 2, 0, 3))
        dma = pltpu.SemaphoreType.DMA
        shape = (H, W, CB, LANES)
        vmem, hbm = pl.BlockSpec(memory_space=pltpu.VMEM), pl.BlockSpec(memory_space=pl.ANY)
        early, z = pl.pallas_call(
            kernel,
            out_shape=(pltpu.VMEM((SPLIT, W, CB, LANES), jnp.bfloat16),
                       pltpu.VMEM((H, PAIRS, TP, N_LOC, LANES), jnp.bfloat16)),
            in_specs=[pl.BlockSpec(memory_space=pl.ANY), pl.BlockSpec(memory_space=pl.ANY),
                      pl.BlockSpec(memory_space=pl.ANY), pl.BlockSpec(memory_space=pl.ANY)],
            out_specs=(vmem, vmem),
            scratch_shapes=[
                pltpu.VMEM((H + 2, W + 2, N_LOC, C), jnp.bfloat16),
                pltpu.VMEM((2, 9, TP, C // TP, LANES), jnp.bfloat16),
                pltpu.VMEM((TP, 8, LANES), jnp.float32),
                dma((H,)), dma((2,)), dma((4, 3)), dma((4, TP)), dma((TP,)), dma((TP,)), dma((H, TP)), dma((H, TP)),
                dma((2, TP)), dma((2, TP)), pltpu.VMEM((2, 1, CB), jnp.float32), dma((2,)), pltpu.SemaphoreType.REGULAR,
            ],
            compiler_params=pltpu.CompilerParams(collective_id=0, has_side_effects=True, vmem_limit_bytes=44040192),
        )(x, w.reshape(9, C // TP, C), scale.reshape(1, CB), shift.reshape(1, CB))
        small = pltpu.CompilerParams(vmem_limit_bytes=2**20)
        written = (jax.ShapeDtypeStruct(shape, jnp.bfloat16), jax.ShapeDtypeStruct((8, LANES), jnp.float32))
        out, token = pl.pallas_call(
            functools.partial(write, 0, SPLIT, 4), out_shape=written, in_specs=[vmem], out_specs=(hbm, hbm), scratch_shapes=[dma((SPLIT // 4,))], compiler_params=small)(early)
        late = pl.pallas_call(
            finish,
            out_shape=pltpu.VMEM((LATE, W, CB, LANES), jnp.bfloat16),
            in_specs=[vmem, hbm],
            out_specs=vmem,
            scratch_shapes=[
                pltpu.VMEM((LATE, PAIRS, TP, N_LOC, LANES), jnp.bfloat16),
                dma((LATE, TP)), dma((LATE, TP)), dma((3, TP)), dma((3, TP)), pltpu.SemaphoreType.REGULAR((2,)),
            ],
            compiler_params=pltpu.CompilerParams(collective_id=1, has_side_effects=True, vmem_limit_bytes=12 * 2**20),
        )(z, token)
        out, _ = pl.pallas_call(
            functools.partial(write, SPLIT, LATE, 2), out_shape=written, in_specs=[vmem, hbm], out_specs=(hbm, hbm), scratch_shapes=[dma((LATE // 2,))], input_output_aliases={1: 0}, compiler_params=small)(late, out)
        return jnp.transpose(out, (3, 0, 1, 2))

    return jax.shard_map(local_step, mesh=mesh, in_specs=(P(("pp", "tp")), P(None, None, "tp", None), P("tp"), P("tp")),
                         out_specs=P("pp", None, None, "tp"), check_vma=False)
```

```python
import functools

import jax
import jax.numpy as jnp
from jax import lax
from jax.experimental import pallas as pl
from jax.experimental.pallas import tpu as pltpu
from jax.sharding import PartitionSpec as P

MESH = pl.DeviceIdType.MESH
H, W, C = 28, 28, 256
N_LOC = 32
TP = 4
CB = C // TP
LANES = 128
PAIRS = W // 2
Q = 7
G = 4
GROUPS = H // G
LAST = H - 1
SOON, LATER = 1, 0
SPLIT = 23
LATER_SPLIT = 27
LATE = H - SPLIT
PARTS = ((0, 3, 3), (0, 6, 3), (0, 0, 3), (1, 0, 9))
ORDER = (1, 0)
FIRST = ((0, 0), (1, 0), (0, 1), (1, 1))
REST = ((2, 0), (2, 1), (3, 0), (3, 1))
HEAD = ((0, 7), (7, 7))
ROWS = ((1, 1), (2, 2), (4, 4), (8, 8), (16, 7))
LATER_ROWS = (SPLIT, LATER_SPLIT - SPLIT)
LATE_SOON = ((0, 4),)
LATE_LATER = ()
TAIL = ((0, 7), (7, 5), (12, 2))


def kernel(act, w, scale, shift, out, buf, xpad, wf, sb, xsem, wlsem, wssem, wrsem, bssem, brsem, ssem, rsem, esem, fsem, vecs, vsem, ready):
    pp, tp = lax.axis_index("pp"), lax.axis_index("tp")
    chip, core = tp // 2, tp % 2
    far = 1 - chip

    def half_of(sel, receiver):
        return receiver if sel == 0 else 1 - receiver

    def w_local(half):
        return pltpu.make_async_copy(
            w.at[:, :, pl.ds(pl.multiple_of(half * LANES, LANES), LANES)], wf.at[half, :, tp], wlsem.at[half])

    def w_copy(part, owner, slot, target):
        sel, tap, taps = PARTS[part]
        block = wf.at[half_of(sel, target // 2), pl.ds(tap, taps), owner]
        return pltpu.make_async_remote_copy(
            src_ref=block, dst_ref=block, send_sem=wssem.at[part, slot], recv_sem=wrsem.at[part, owner],
            device_id=(0, target), device_id_type=MESH)

    def x_copy(h):
        return pltpu.make_async_copy(act.at[h], xpad.at[h + 1, pl.ds(1, W)], xsem.at[h])

    def vec_copy(i):
        return pltpu.make_async_copy((scale, shift)[i], vecs.at[i], vsem.at[i])

    def b_copy(k, owner):
        return pltpu.make_async_remote_copy(
            src_ref=sb.at[tp], dst_ref=sb.at[tp], send_sem=bssem.at[k], recv_sem=brsem.at[owner],
            device_id=(0, lax.rem(tp + k, TP)), device_id_type=MESH)

    def z_copy(h, rows, t, owner):
        return pltpu.make_async_remote_copy(
            src_ref=buf.at[pl.ds(h, rows), :, t], dst_ref=buf.at[pl.ds(h, rows), :, owner],
            send_sem=ssem.at[h, t], recv_sem=rsem.at[h, owner], device_id=(1, t), device_id_type=MESH)

    def z_head(q, t, owner):
        return pltpu.make_async_remote_copy(
            src_ref=buf.at[0, pl.ds(*HEAD[q]), t], dst_ref=buf.at[0, pl.ds(*HEAD[q]), owner],
            send_sem=esem.at[q, t], recv_sem=fsem.at[q, owner], device_id=(1, t), device_id_type=MESH)

    barrier = pltpu.get_barrier_semaphore()

    @pl.when(pp == 0)
    def _():
        for k in range(1, TP):
            pl.semaphore_signal(barrier, inc=1, device_id=(0, lax.rem(tp + k, TP)), device_id_type=MESH)
        for k in range(TP):
            pl.semaphore_signal(barrier, inc=1, device_id=(1, lax.rem(tp + k, TP)), device_id_type=MESH)

    helps = jnp.logical_and(pp == 1, core == 1)
    has_w = jnp.logical_or(pp == 0, helps)

    @pl.when(pp == 0)
    def _():
        vec_copy(0).start()
        vec_copy(1).start()

    @pl.when(has_w)
    def _():
        w_local(0).start()
        w_local(1).start()

    @pl.when(pp == 0)
    def _():
        x_copy(0).start()
        x_copy(1).start()
        for i in range(2):
            vec_copy(i).wait()
            sb[tp, i : i + 1, :] = jnp.concatenate([vecs[i], vecs[i]], axis=1)

    pl.semaphore_wait(barrier, TP - 1 + pp)

    @pl.when(pp == 1)
    def _():
        for k in range(TP):
            pl.semaphore_signal(ready, inc=1, device_id=(0, lax.rem(tp + k, TP)), device_id_type=MESH)

    @pl.when(pp == 0)
    def _():
        for k in range(1, TP):
            b_copy(k, tp).start()

    @pl.when(has_w)
    def _():
        w_local(0).wait()
        w_local(1).wait()

    def w_sends(act_on, stages):
        for part, c in stages:
            sends = jnp.logical_or(jnp.logical_and(pp == 0, core == 0), helps)
            if (part, c) == FIRST[0]:
                sends = pp == 0

            @pl.when(sends)
            def _():
                act_on(w_copy(part, tp, c, far * 2 + c))

            if c == 0:
                @pl.when(pp == 0)
                def _():
                    act_on(w_copy(part, tp, 2, chip * 2 + 1 - core))

    w_sends(lambda c: c.start(), FIRST)

    @pl.when(pp == 1)
    def _():
        w_sends(lambda c: c.start(), REST)

    @pl.when(pp == 0)
    def _():
        def start_x(h, _):
            x_copy(h).start()
            return 0
        lax.fori_loop(2, H, start_x, 0)

        zero = jnp.zeros((W + 2, N_LOC, C), jnp.bfloat16)
        xpad[0] = zero
        xpad[H + 1] = zero
        xpad[:, 0] = zero
        xpad[:, W + 1] = zero

        for k in range(1, TP):
            b_copy(k, lax.rem(tp + k, TP)).wait_recv()

        low = lax.broadcasted_iota(jnp.int32, (1, LANES), 1) < CB

        def wait_w(part):
            for k in range(1, TP):
                w_copy(part, lax.rem(tp + k, TP), 0, tp).wait_recv()

        def pixels(h, half, start, count, first_tap):
            sc = jnp.where(low, sb[2 * half, 0:1, :], sb[2 * half + 1, 0:1, :])
            sh = jnp.where(low, sb[2 * half, 1:2, :], sb[2 * half + 1, 1:2, :])

            def conv(w0):
                acc = None
                for tap in range(first_tap, 9):
                    lhs = xpad[h + tap // 3, pl.ds(w0 + tap % 3, count)].reshape(count * N_LOC, C)
                    part = jnp.dot(lhs, wf[half, tap].reshape(C, LANES), preferred_element_type=jnp.float32)
                    acc = part if acc is None else acc + part
                return jnp.maximum(acc * sc + sh, 0.0)

            even, odd = conv(start), conv(PAIRS + start)
            first = jnp.where(low, even, pltpu.roll(odd, CB, 1)).astype(jnp.bfloat16)
            second = jnp.where(low, pltpu.roll(even, CB, 1), odd).astype(jnp.bfloat16)
            buf[h, pl.ds(start, count), 2 * half] = first.reshape(count, N_LOC, LANES)
            buf[h, pl.ds(start, count), 2 * half + 1] = second.reshape(count, N_LOC, LANES)

        x_copy(0).wait()
        x_copy(1).wait()
        wait_w(0)
        wait_w(1)
        for q, (start, count) in enumerate(HEAD):
            pixels(0, chip, start, count, 3)
            if q == 0:
                pl.semaphore_wait(ready, TP)
            for k in ORDER:
                z_head(q, 2 * chip + k, tp).start()
        w_sends(lambda c: c.start(), REST)
        wait_w(2)

        def step(i, _):
            g, r = i // (2 * G), i % (2 * G)
            own = r < G
            half = jnp.where(own, chip, far)
            h = g * G + r % G

            @pl.when(i == G)
            def _():
                wait_w(3)

            @pl.when(jnp.logical_and(own, h < LAST))
            def _():
                x_copy(h + 1).wait()

            for q in range(2):
                pixels(h, half, q * Q, Q, 0)

            def send(first, rows, cores):
                for k in cores:
                    z_copy(first, rows, 2 * half + k, tp).start()

            @pl.when(h == 0)
            def _():
                send(0, 1, (0, 1))

            for first, rows in ROWS[:-1]:
                @pl.when(h == first + rows - 1)
                def _():
                    send(first, rows, (0, 1))

            last = jnp.logical_and(own, core == LATER)

            @pl.when(h == SPLIT - 1)
            def _():
                send(*ROWS[-1], (SOON,))

            @pl.when(jnp.logical_and(h == SPLIT - 1, jnp.logical_not(last)))
            def _():
                send(*ROWS[-1], (LATER,))

            @pl.when(jnp.logical_and(h == LATER_SPLIT - 1, core == LATER))
            def _():
                send(*LATER_ROWS, (SOON,))

            @pl.when(jnp.logical_and(h == LATER_SPLIT - 1, last))
            def _():
                send(*ROWS[-1], (LATER,))

            @pl.when(jnp.logical_and(h == LATER_SPLIT - 1, core == LATER))
            def _():
                send(*LATER_ROWS, (LATER,))
            return 0
        lax.fori_loop(1, 2 * H, step, 0)

        def clear(h, _):
            out[h] = jnp.zeros((W, CB, LANES), jnp.bfloat16)
            return 0
        lax.fori_loop(0, SPLIT, clear, 0)

        for k in range(1, TP):
            b_copy(k, tp).wait_send()

    w_sends(lambda c: c.wait_send(), FIRST + REST)

    @pl.when(pp == 0)
    def _():
        for k in range(2):
            for q in range(len(HEAD)):
                z_head(q, 2 * chip + k, tp).wait_send()
            z_copy(0, 1, 2 * far + k, tp).wait_send()
        for t in range(TP):
            for first, rows in ROWS:
                z_copy(first, rows, t, tp).wait_send()

            @pl.when(core == LATER)
            def _():
                z_copy(*LATER_ROWS, t, tp).wait_send()

    @pl.when(pp == 1)
    def _():
        def turn_rows(first, rows):
            def row(h, _):
                for p in range(PAIRS):
                    turn(buf[h, p].reshape(LANES, LANES), out, h, p)
                return 0
            lax.fori_loop(first, first + rows, row, 0)

        for k in range(2):
            for q in range(len(HEAD)):
                z_head(q, 2 * chip + k, 2 * chip + k).wait_recv()
            z_copy(0, 1, 2 * far + k, 2 * far + k).wait_recv()
        turn_rows(0, 1)
        for first, rows in ROWS:
            for s in range(TP):
                z_copy(first, rows, s, s).wait_recv()
            turn_rows(first, rows)
        for s in (LATER, 2 + LATER):
            z_copy(*LATER_ROWS, s, s).wait_recv()


def turn(block, out, h, p):
    turned = block.T
    out[h, p] = turned[:CB]
    out[h, p + PAIRS] = turned[CB:]


def finish(z, _, out, got, ssem, rsem, tsem, usem, ready):
    pp, tp = lax.axis_index("pp"), lax.axis_index("tp")
    core = tp % 2
    source = pp == 0
    soon = core == SOON

    def z_copy(first, rows, t, owner):
        return pltpu.make_async_remote_copy(
            src_ref=z.at[pl.ds(SPLIT + first, rows), :, t], dst_ref=got.at[pl.ds(first, rows), :, owner],
            send_sem=ssem.at[first, t], recv_sem=rsem.at[first, owner], device_id=(1, t), device_id_type=MESH)

    def z_tail(q, t, owner):
        return pltpu.make_async_remote_copy(
            src_ref=z.at[LAST, pl.ds(*TAIL[q]), t], dst_ref=got.at[LATE - 1, pl.ds(*TAIL[q]), owner],
            send_sem=tsem.at[q, t], recv_sem=usem.at[q, owner], device_id=(1, t), device_id_type=MESH)

    def copies(rows, t, owner):
        return [z_copy(*r, t, owner) for r in rows] + [z_tail(q, t, owner) for q in range(len(TAIL))]

    barrier = pltpu.get_barrier_semaphore()

    def greet(where, targets):
        @pl.when(where)
        def _():
            for target in targets:
                pl.semaphore_signal(barrier, inc=1, device_id=target, device_id_type=MESH)

    greet(source & soon, [(1, 0), (1, 1), (1, 2), (1, 3), (0, lax.rem(tp + 2, TP))])
    greet(source & ~soon, [(1, LATER), (1, 2 + LATER)])
    greet(~source & soon, [(0, LATER), (0, 2 + LATER)])
    pl.semaphore_wait(barrier, jnp.where(source, jnp.where(soon, 1, 2), jnp.where(soon, 2, 4)))

    @pl.when(~source & soon)
    def _():
        for t in (SOON, 2 + SOON):
            pl.semaphore_signal(ready.at[0], inc=1, device_id=(0, t), device_id_type=MESH)

    @pl.when(~source & ~soon)
    def _():
        for t in range(TP):
            pl.semaphore_signal(ready.at[1], inc=1, device_id=(0, t), device_id_type=MESH)

    def sends(rows, k):
        for a in zip(*[copies(rows, t, tp) for t in (k, 2 + k)]):
            for c in a:
                c.start()

    @pl.when(source & soon)
    def _():
        pl.semaphore_wait(ready.at[0], 2)
        sends(LATE_SOON, SOON)
        pl.semaphore_wait(ready.at[1], 2)
        sends(LATE_SOON, LATER)

    @pl.when(source & ~soon)
    def _():
        sends(LATE_LATER, SOON)
        pl.semaphore_wait(ready.at[1], 2)
        sends(LATE_LATER, LATER)

    @pl.when(source)
    def _():
        def clear(h, _):
            out[h] = jnp.zeros((W, CB, LANES), jnp.bfloat16)
            return 0
        lax.fori_loop(0, LATE, clear, 0)
        for rows, where in ((LATE_SOON, soon), (LATE_LATER, ~soon)):
            @pl.when(where)
            def _():
                for t in range(TP):
                    for c in copies(rows, t, tp):
                        c.wait_send()

    @pl.when(~source)
    def _():
        for s in (SOON, 2 + SOON):
            z_copy(*LATE_SOON[0], s, s).wait_recv()

        def mixed(h, _):
            for p in range(PAIRS):
                parts = [got[h, p, s] if s % 2 == SOON else z[SPLIT + h, p, s] for s in range(TP)]
                turn(jnp.concatenate(parts, axis=0), out, h, p)
            return 0
        lax.fori_loop(0, LATER_SPLIT - SPLIT, mixed, 0)
        for first, rows in LATE_LATER:
            for s in range(TP):
                z_copy(first, rows, s, s).wait_recv()

            def row(h, _):
                for p in range(PAIRS):
                    turn(got[h, p].reshape(LANES, LANES), out, h, p)
                return 0
            lax.fori_loop(first, first + rows, row, 0)
        for q, (start, count) in enumerate(TAIL):
            for s in range(TP):
                z_tail(q, s, s).wait_recv()
            for p in range(start, start + count):
                turn(got[LATE - 1, p].reshape(LANES, LANES), out, LATE - 1, p)


def write(first, rows, each, src, *refs):
    dst, _, sem = refs[-3:]
    copies = [pltpu.make_async_copy(src.at[pl.ds(i * each, each)], dst.at[pl.ds(first + i * each, each)], sem.at[i])
              for i in range(rows // each)]
    for c in copies:
        c.start()
    for c in copies:
        c.wait()


def solution(mesh):
    def local_step(act, w, scale, shift):
        x = jnp.transpose(act, (1, 2, 0, 3))
        dma = pltpu.SemaphoreType.DMA
        shape = (H, W, CB, LANES)
        vmem, hbm = pl.BlockSpec(memory_space=pltpu.VMEM), pl.BlockSpec(memory_space=pl.ANY)
        early, z = pl.pallas_call(
            kernel,
            out_shape=(pltpu.VMEM((SPLIT, W, CB, LANES), jnp.bfloat16),
                       pltpu.VMEM((H, PAIRS, TP, N_LOC, LANES), jnp.bfloat16)),
            in_specs=[pl.BlockSpec(memory_space=pl.ANY), pl.BlockSpec(memory_space=pl.ANY),
                      pl.BlockSpec(memory_space=pl.ANY), pl.BlockSpec(memory_space=pl.ANY)],
            out_specs=(vmem, vmem),
            scratch_shapes=[
                pltpu.VMEM((H + 2, W + 2, N_LOC, C), jnp.bfloat16),
                pltpu.VMEM((2, 9, TP, C // TP, LANES), jnp.bfloat16),
                pltpu.VMEM((TP, 8, LANES), jnp.float32),
                dma((H,)), dma((2,)), dma((4, 3)), dma((4, TP)), dma((TP,)), dma((TP,)), dma((H, TP)), dma((H, TP)),
                dma((2, TP)), dma((2, TP)), pltpu.VMEM((2, 1, CB), jnp.float32), dma((2,)), pltpu.SemaphoreType.REGULAR,
            ],
            compiler_params=pltpu.CompilerParams(collective_id=0, has_side_effects=True, vmem_limit_bytes=42677043),
        )(x, w.reshape(9, C // TP, C), scale.reshape(1, CB), shift.reshape(1, CB))
        small = pltpu.CompilerParams(vmem_limit_bytes=2**20)
        written = (jax.ShapeDtypeStruct(shape, jnp.bfloat16), jax.ShapeDtypeStruct((8, LANES), jnp.float32))
        out, token = pl.pallas_call(
            functools.partial(write, 0, SPLIT, 1), out_shape=written, in_specs=[vmem], out_specs=(hbm, hbm), scratch_shapes=[dma((SPLIT // 1,))], compiler_params=small)(early)
        late = pl.pallas_call(
            finish,
            out_shape=pltpu.VMEM((LATE, W, CB, LANES), jnp.bfloat16),
            in_specs=[vmem, hbm],
            out_specs=vmem,
            scratch_shapes=[
                pltpu.VMEM((LATE, PAIRS, TP, N_LOC, LANES), jnp.bfloat16),
                dma((LATE, TP)), dma((LATE, TP)), dma((3, TP)), dma((3, TP)), pltpu.SemaphoreType.REGULAR((2,)),
            ],
            compiler_params=pltpu.CompilerParams(collective_id=1, has_side_effects=True, vmem_limit_bytes=12 * 2**20),
        )(z, token)
        out, _ = pl.pallas_call(
            functools.partial(write, SPLIT, LATE, 1), out_shape=written, in_specs=[vmem, hbm], out_specs=(hbm, hbm), scratch_shapes=[dma((LATE // 1,))], input_output_aliases={1: 0}, compiler_params=small)(late, out)
        return jnp.transpose(out, (3, 0, 1, 2))

    return jax.shard_map(local_step, mesh=mesh, in_specs=(P(("pp", "tp")), P(None, None, "tp", None), P("tp"), P("tp")),
                         out_specs=P("pp", None, None, "tp"), check_vma=False)
```

```python
import functools

import jax
import jax.numpy as jnp
from jax import lax
from jax.experimental import pallas as pl
from jax.experimental.pallas import tpu as pltpu
from jax.sharding import PartitionSpec as P

MESH = pl.DeviceIdType.MESH
H, W, C = 28, 28, 256
N_LOC = 32
TP = 4
CB = C // TP
LANES = 128
PAIRS = W // 2
Q = 7
G = 4
GROUPS = H // G
LAST = H - 1
SOON, LATER = 1, 0
SPLIT = 23
LATER_SPLIT = 27
LATE = H - SPLIT
PARTS = ((0, 3, 3), (0, 6, 3), (0, 0, 3), (1, 0, 9))
ORDER = (1, 0)
FIRST = ((0, 0), (1, 0), (0, 1), (1, 1))
REST = ((2, 0), (2, 1), (3, 0), (3, 1))
HEAD = ((0, 7), (7, 7))
ROWS = ((1, 1), (2, 6), (8, 15))
LATER_ROWS = (SPLIT, LATER_SPLIT - SPLIT)
LATE_SOON = ((0, 4),)
LATE_LATER = ()
TAIL = ((0, 12), (12, 2))


def kernel(act, w, scale, shift, out, buf, xpad, wf, sb, xsem, wlsem, wssem, wrsem, bssem, brsem, ssem, rsem, esem, fsem, vecs, vsem, ready):
    pp, tp = lax.axis_index("pp"), lax.axis_index("tp")
    chip, core = tp // 2, tp % 2
    far = 1 - chip

    def half_of(sel, receiver):
        return receiver if sel == 0 else 1 - receiver

    def w_local(half):
        return pltpu.make_async_copy(
            w.at[:, :, pl.ds(pl.multiple_of(half * LANES, LANES), LANES)], wf.at[half, :, tp], wlsem.at[half])

    def w_copy(part, owner, slot, target):
        sel, tap, taps = PARTS[part]
        block = wf.at[half_of(sel, target // 2), pl.ds(tap, taps), owner]
        return pltpu.make_async_remote_copy(
            src_ref=block, dst_ref=block, send_sem=wssem.at[part, slot], recv_sem=wrsem.at[part, owner],
            device_id=(0, target), device_id_type=MESH)

    def x_copy(h):
        return pltpu.make_async_copy(act.at[h], xpad.at[h + 1, pl.ds(1, W)], xsem.at[h])

    def vec_copy(i):
        return pltpu.make_async_copy((scale, shift)[i], vecs.at[i], vsem.at[i])

    def b_copy(k, owner):
        return pltpu.make_async_remote_copy(
            src_ref=sb.at[tp], dst_ref=sb.at[tp], send_sem=bssem.at[k], recv_sem=brsem.at[owner],
            device_id=(0, lax.rem(tp + k, TP)), device_id_type=MESH)

    def z_copy(h, rows, t, owner):
        return pltpu.make_async_remote_copy(
            src_ref=buf.at[pl.ds(h, rows), :, t], dst_ref=buf.at[pl.ds(h, rows), :, owner],
            send_sem=ssem.at[h, t], recv_sem=rsem.at[h, owner], device_id=(1, t), device_id_type=MESH)

    def z_head(q, t, owner):
        return pltpu.make_async_remote_copy(
            src_ref=buf.at[0, pl.ds(*HEAD[q]), t], dst_ref=buf.at[0, pl.ds(*HEAD[q]), owner],
            send_sem=esem.at[q, t], recv_sem=fsem.at[q, owner], device_id=(1, t), device_id_type=MESH)

    barrier = pltpu.get_barrier_semaphore()

    @pl.when(pp == 0)
    def _():
        for k in range(1, TP):
            pl.semaphore_signal(barrier, inc=1, device_id=(0, lax.rem(tp + k, TP)), device_id_type=MESH)
        for k in range(TP):
            pl.semaphore_signal(barrier, inc=1, device_id=(1, lax.rem(tp + k, TP)), device_id_type=MESH)

    helps = jnp.logical_and(pp == 1, core == 1)
    has_w = jnp.logical_or(pp == 0, helps)

    @pl.when(pp == 0)
    def _():
        vec_copy(0).start()
        vec_copy(1).start()

    @pl.when(has_w)
    def _():
        w_local(0).start()
        w_local(1).start()

    @pl.when(pp == 0)
    def _():
        x_copy(0).start()
        x_copy(1).start()
        for i in range(2):
            vec_copy(i).wait()
            sb[tp, i : i + 1, :] = jnp.concatenate([vecs[i], vecs[i]], axis=1)

    pl.semaphore_wait(barrier, TP - 1 + pp)

    @pl.when(pp == 1)
    def _():
        for k in range(TP):
            pl.semaphore_signal(ready, inc=1, device_id=(0, lax.rem(tp + k, TP)), device_id_type=MESH)

    @pl.when(pp == 0)
    def _():
        for k in range(1, TP):
            b_copy(k, tp).start()

    @pl.when(has_w)
    def _():
        w_local(0).wait()
        w_local(1).wait()

    def w_sends(act_on, stages):
        for part, c in stages:
            sends = jnp.logical_or(jnp.logical_and(pp == 0, core == 0), helps)
            if (part, c) == FIRST[0]:
                sends = pp == 0

            @pl.when(sends)
            def _():
                act_on(w_copy(part, tp, c, far * 2 + c))

            if c == 0:
                @pl.when(pp == 0)
                def _():
                    act_on(w_copy(part, tp, 2, chip * 2 + 1 - core))

    w_sends(lambda c: c.start(), FIRST)

    @pl.when(pp == 1)
    def _():
        w_sends(lambda c: c.start(), REST)

    @pl.when(pp == 0)
    def _():
        def start_x(h, _):
            x_copy(h).start()
            return 0
        lax.fori_loop(2, H, start_x, 0)

        zero = jnp.zeros((W + 2, N_LOC, C), jnp.bfloat16)
        xpad[0] = zero
        xpad[H + 1] = zero
        xpad[:, 0] = zero
        xpad[:, W + 1] = zero

        for k in range(1, TP):
            b_copy(k, lax.rem(tp + k, TP)).wait_recv()

        low = lax.broadcasted_iota(jnp.int32, (1, LANES), 1) < CB

        def wait_w(part):
            for k in range(1, TP):
                w_copy(part, lax.rem(tp + k, TP), 0, tp).wait_recv()

        def pixels(h, half, start, count, first_tap):
            sc = jnp.where(low, sb[2 * half, 0:1, :], sb[2 * half + 1, 0:1, :])
            sh = jnp.where(low, sb[2 * half, 1:2, :], sb[2 * half + 1, 1:2, :])

            def conv(w0):
                acc = None
                for tap in range(first_tap, 9):
                    lhs = xpad[h + tap // 3, pl.ds(w0 + tap % 3, count)].reshape(count * N_LOC, C)
                    part = jnp.dot(lhs, wf[half, tap].reshape(C, LANES), preferred_element_type=jnp.float32)
                    acc = part if acc is None else acc + part
                return jnp.maximum(acc * sc + sh, 0.0)

            even, odd = conv(start), conv(PAIRS + start)
            first = jnp.where(low, even, pltpu.roll(odd, CB, 1)).astype(jnp.bfloat16)
            second = jnp.where(low, pltpu.roll(even, CB, 1), odd).astype(jnp.bfloat16)
            buf[h, pl.ds(start, count), 2 * half] = first.reshape(count, N_LOC, LANES)
            buf[h, pl.ds(start, count), 2 * half + 1] = second.reshape(count, N_LOC, LANES)

        x_copy(0).wait()
        x_copy(1).wait()
        wait_w(0)
        wait_w(1)
        for q, (start, count) in enumerate(HEAD):
            pixels(0, chip, start, count, 3)
            if q == 0:
                pl.semaphore_wait(ready, TP)
            for k in ORDER:
                z_head(q, 2 * chip + k, tp).start()
        w_sends(lambda c: c.start(), REST)
        wait_w(2)

        def step(i, _):
            g, r = i // (2 * G), i % (2 * G)
            own = r < G
            half = jnp.where(own, chip, far)
            h = g * G + r % G

            @pl.when(i == G)
            def _():
                wait_w(3)

            @pl.when(jnp.logical_and(own, h < LAST))
            def _():
                x_copy(h + 1).wait()

            for q in range(2):
                pixels(h, half, q * Q, Q, 0)

            def send(first, rows, cores):
                for k in cores:
                    z_copy(first, rows, 2 * half + k, tp).start()

            @pl.when(h == 0)
            def _():
                send(0, 1, (0, 1))

            for first, rows in ROWS[:-1]:
                @pl.when(h == first + rows - 1)
                def _():
                    send(first, rows, (0, 1))

            last = jnp.logical_and(own, core == LATER)

            @pl.when(h == SPLIT - 1)
            def _():
                send(*ROWS[-1], (SOON,))

            @pl.when(jnp.logical_and(h == SPLIT - 1, jnp.logical_not(last)))
            def _():
                send(*ROWS[-1], (LATER,))

            @pl.when(jnp.logical_and(h == LATER_SPLIT - 1, core == LATER))
            def _():
                send(*LATER_ROWS, (SOON,))

            @pl.when(jnp.logical_and(h == LATER_SPLIT - 1, last))
            def _():
                send(*ROWS[-1], (LATER,))

            @pl.when(jnp.logical_and(h == LATER_SPLIT - 1, core == LATER))
            def _():
                send(*LATER_ROWS, (LATER,))
            return 0
        lax.fori_loop(1, 2 * H, step, 0)

        def clear(h, _):
            out[h] = jnp.zeros((W, CB, LANES), jnp.bfloat16)
            return 0
        lax.fori_loop(0, SPLIT, clear, 0)

        for k in range(1, TP):
            b_copy(k, tp).wait_send()

    w_sends(lambda c: c.wait_send(), FIRST + REST)

    @pl.when(pp == 0)
    def _():
        for k in range(2):
            for q in range(len(HEAD)):
                z_head(q, 2 * chip + k, tp).wait_send()
            z_copy(0, 1, 2 * far + k, tp).wait_send()
        for t in range(TP):
            for first, rows in ROWS:
                z_copy(first, rows, t, tp).wait_send()

            @pl.when(core == LATER)
            def _():
                z_copy(*LATER_ROWS, t, tp).wait_send()

    @pl.when(pp == 1)
    def _():
        def turn_rows(first, rows):
            def row(h, _):
                for p in range(PAIRS):
                    turn(buf[h, p].reshape(LANES, LANES), out, h, p)
                return 0
            lax.fori_loop(first, first + rows, row, 0)

        for k in range(2):
            for q in range(len(HEAD)):
                z_head(q, 2 * chip + k, 2 * chip + k).wait_recv()
            z_copy(0, 1, 2 * far + k, 2 * far + k).wait_recv()
        turn_rows(0, 1)
        for first, rows in ROWS:
            for s in range(TP):
                z_copy(first, rows, s, s).wait_recv()
            turn_rows(first, rows)
        for s in (LATER, 2 + LATER):
            z_copy(*LATER_ROWS, s, s).wait_recv()


def turn(block, out, h, p):
    turned = block.T
    out[h, p] = turned[:CB]
    out[h, p + PAIRS] = turned[CB:]


def finish(z, _, out, got, ssem, rsem, tsem, usem, ready):
    pp, tp = lax.axis_index("pp"), lax.axis_index("tp")
    core = tp % 2
    source = pp == 0
    soon = core == SOON

    def z_copy(first, rows, t, owner):
        return pltpu.make_async_remote_copy(
            src_ref=z.at[pl.ds(SPLIT + first, rows), :, t], dst_ref=got.at[pl.ds(first, rows), :, owner],
            send_sem=ssem.at[first, t], recv_sem=rsem.at[first, owner], device_id=(1, t), device_id_type=MESH)

    def z_tail(q, t, owner):
        return pltpu.make_async_remote_copy(
            src_ref=z.at[LAST, pl.ds(*TAIL[q]), t], dst_ref=got.at[LATE - 1, pl.ds(*TAIL[q]), owner],
            send_sem=tsem.at[q, t], recv_sem=usem.at[q, owner], device_id=(1, t), device_id_type=MESH)

    def copies(rows, t, owner):
        return [z_copy(*r, t, owner) for r in rows] + [z_tail(q, t, owner) for q in range(len(TAIL))]

    barrier = pltpu.get_barrier_semaphore()

    def greet(where, targets):
        @pl.when(where)
        def _():
            for target in targets:
                pl.semaphore_signal(barrier, inc=1, device_id=target, device_id_type=MESH)

    greet(source & soon, [(1, 0), (1, 1), (1, 2), (1, 3), (0, lax.rem(tp + 2, TP))])
    greet(source & ~soon, [(1, LATER), (1, 2 + LATER)])
    greet(~source & soon, [(0, LATER), (0, 2 + LATER)])
    pl.semaphore_wait(barrier, jnp.where(source, jnp.where(soon, 1, 2), jnp.where(soon, 2, 4)))

    @pl.when(~source & soon)
    def _():
        for t in (SOON, 2 + SOON):
            pl.semaphore_signal(ready.at[0], inc=1, device_id=(0, t), device_id_type=MESH)

    @pl.when(~source & ~soon)
    def _():
        for t in range(TP):
            pl.semaphore_signal(ready.at[1], inc=1, device_id=(0, t), device_id_type=MESH)

    def sends(rows, k):
        for a in zip(*[copies(rows, t, tp) for t in (k, 2 + k)]):
            for c in a:
                c.start()

    @pl.when(source & soon)
    def _():
        pl.semaphore_wait(ready.at[0], 2)
        sends(LATE_SOON, SOON)
        pl.semaphore_wait(ready.at[1], 2)
        sends(LATE_SOON, LATER)

    @pl.when(source & ~soon)
    def _():
        sends(LATE_LATER, SOON)
        pl.semaphore_wait(ready.at[1], 2)
        sends(LATE_LATER, LATER)

    @pl.when(source)
    def _():
        def clear(h, _):
            out[h] = jnp.zeros((W, CB, LANES), jnp.bfloat16)
            return 0
        lax.fori_loop(0, LATE, clear, 0)
        for rows, where in ((LATE_SOON, soon), (LATE_LATER, ~soon)):
            @pl.when(where)
            def _():
                for t in range(TP):
                    for c in copies(rows, t, tp):
                        c.wait_send()

    @pl.when(~source)
    def _():
        for s in (SOON, 2 + SOON):
            z_copy(*LATE_SOON[0], s, s).wait_recv()

        def mixed(h, _):
            for p in range(PAIRS):
                parts = [got[h, p, s] if s % 2 == SOON else z[SPLIT + h, p, s] for s in range(TP)]
                turn(jnp.concatenate(parts, axis=0), out, h, p)
            return 0
        lax.fori_loop(0, LATER_SPLIT - SPLIT, mixed, 0)
        for first, rows in LATE_LATER:
            for s in range(TP):
                z_copy(first, rows, s, s).wait_recv()

            def row(h, _):
                for p in range(PAIRS):
                    turn(got[h, p].reshape(LANES, LANES), out, h, p)
                return 0
            lax.fori_loop(first, first + rows, row, 0)
        for q, (start, count) in enumerate(TAIL):
            for s in range(TP):
                z_tail(q, s, s).wait_recv()
            for p in range(start, start + count):
                turn(got[LATE - 1, p].reshape(LANES, LANES), out, LATE - 1, p)


def write(first, rows, each, src, *refs):
    dst, _, sem = refs[-3:]
    copies = [pltpu.make_async_copy(src.at[pl.ds(i * each, each)], dst.at[pl.ds(first + i * each, each)], sem.at[i])
              for i in range(rows // each)]
    for c in copies:
        c.start()
    for c in copies:
        c.wait()


def solution(mesh):
    def local_step(act, w, scale, shift):
        x = jnp.transpose(act, (1, 2, 0, 3))
        dma = pltpu.SemaphoreType.DMA
        shape = (H, W, CB, LANES)
        vmem, hbm = pl.BlockSpec(memory_space=pltpu.VMEM), pl.BlockSpec(memory_space=pl.ANY)
        early, z = pl.pallas_call(
            kernel,
            out_shape=(pltpu.VMEM((SPLIT, W, CB, LANES), jnp.bfloat16),
                       pltpu.VMEM((H, PAIRS, TP, N_LOC, LANES), jnp.bfloat16)),
            in_specs=[pl.BlockSpec(memory_space=pl.ANY), pl.BlockSpec(memory_space=pl.ANY),
                      pl.BlockSpec(memory_space=pl.ANY), pl.BlockSpec(memory_space=pl.ANY)],
            out_specs=(vmem, vmem),
            scratch_shapes=[
                pltpu.VMEM((H + 2, W + 2, N_LOC, C), jnp.bfloat16),
                pltpu.VMEM((2, 9, TP, C // TP, LANES), jnp.bfloat16),
                pltpu.VMEM((TP, 8, LANES), jnp.float32),
                dma((H,)), dma((2,)), dma((4, 3)), dma((4, TP)), dma((TP,)), dma((TP,)), dma((H, TP)), dma((H, TP)),
                dma((2, TP)), dma((2, TP)), pltpu.VMEM((2, 1, CB), jnp.float32), dma((2,)), pltpu.SemaphoreType.REGULAR,
            ],
            compiler_params=pltpu.CompilerParams(collective_id=0, has_side_effects=True, vmem_limit_bytes=42677043),
        )(x, w.reshape(9, C // TP, C), scale.reshape(1, CB), shift.reshape(1, CB))
        small = pltpu.CompilerParams(vmem_limit_bytes=2**20)
        written = (jax.ShapeDtypeStruct(shape, jnp.bfloat16), jax.ShapeDtypeStruct((8, LANES), jnp.float32))
        out, token = pl.pallas_call(
            functools.partial(write, 0, SPLIT, 1), out_shape=written, in_specs=[vmem], out_specs=(hbm, hbm), scratch_shapes=[dma((SPLIT // 1,))], compiler_params=small)(early)
        late = pl.pallas_call(
            finish,
            out_shape=pltpu.VMEM((LATE, W, CB, LANES), jnp.bfloat16),
            in_specs=[vmem, hbm],
            out_specs=vmem,
            scratch_shapes=[
                pltpu.VMEM((LATE, PAIRS, TP, N_LOC, LANES), jnp.bfloat16),
                dma((LATE, TP)), dma((LATE, TP)), dma((2, TP)), dma((2, TP)), pltpu.SemaphoreType.REGULAR((2,)),
            ],
            compiler_params=pltpu.CompilerParams(collective_id=1, has_side_effects=True, vmem_limit_bytes=12 * 2**20),
        )(z, token)
        out, _ = pl.pallas_call(
            functools.partial(write, SPLIT, LATE, 1), out_shape=written, in_specs=[vmem, hbm], out_specs=(hbm, hbm), scratch_shapes=[dma((LATE // 1,))], input_output_aliases={1: 0}, compiler_params=small)(late, out)
        return jnp.transpose(out, (3, 0, 1, 2))

    return jax.shard_map(local_step, mesh=mesh, in_specs=(P(("pp", "tp")), P(None, None, "tp", None), P("tp"), P("tp")),
                         out_specs=P("pp", None, None, "tp"), check_vma=False)
```

```python
import functools

import jax
import jax.numpy as jnp
from jax import lax
from jax.experimental import pallas as pl
from jax.experimental.pallas import tpu as pltpu
from jax.sharding import PartitionSpec as P

MESH = pl.DeviceIdType.MESH
H, W, C = 28, 28, 256
N_LOC = 32
TP = 4
CB = C // TP
LANES = 128
PAIRS = W // 2
Q = 7
G = 4
GROUPS = H // G
LAST = H - 1
SOON, LATER = 1, 0
SPLIT = 23
LATER_SPLIT = 27
LATE = H - SPLIT
PARTS = ((0, 3, 3), (0, 6, 3), (0, 0, 3), (1, 0, 9))
ORDER = (1, 0)
FIRST = ((0, 0), (1, 0), (0, 1), (1, 1))
REST = ((2, 0), (2, 1), (3, 0), (3, 1))
HEAD = ((0, 2), (2, 12))
ROWS = ((1, 1), (2, 6), (8, 15))
LATER_ROWS = (SPLIT, LATER_SPLIT - SPLIT)
LATE_SOON = ((0, 2), (2, 2))
LATE_LATER = ()
TAIL = ((0, 12), (12, 2))


def kernel(act, w, scale, shift, out, buf, xpad, wf, sb, xsem, wlsem, wssem, wrsem, bssem, brsem, ssem, rsem, esem, fsem, vecs, vsem, ready):
    pp, tp = lax.axis_index("pp"), lax.axis_index("tp")
    chip, core = tp // 2, tp % 2
    far = 1 - chip

    def half_of(sel, receiver):
        return receiver if sel == 0 else 1 - receiver

    def w_local(half):
        return pltpu.make_async_copy(
            w.at[:, :, pl.ds(pl.multiple_of(half * LANES, LANES), LANES)], wf.at[half, :, tp], wlsem.at[half])

    def w_copy(part, owner, slot, target):
        sel, tap, taps = PARTS[part]
        block = wf.at[half_of(sel, target // 2), pl.ds(tap, taps), owner]
        return pltpu.make_async_remote_copy(
            src_ref=block, dst_ref=block, send_sem=wssem.at[part, slot], recv_sem=wrsem.at[part, owner],
            device_id=(0, target), device_id_type=MESH)

    def x_copy(h):
        return pltpu.make_async_copy(act.at[h], xpad.at[h + 1, pl.ds(1, W)], xsem.at[h])

    def vec_copy(i):
        return pltpu.make_async_copy((scale, shift)[i], vecs.at[i], vsem.at[i])

    def b_copy(k, owner):
        return pltpu.make_async_remote_copy(
            src_ref=sb.at[tp], dst_ref=sb.at[tp], send_sem=bssem.at[k], recv_sem=brsem.at[owner],
            device_id=(0, lax.rem(tp + k, TP)), device_id_type=MESH)

    def z_copy(h, rows, t, owner):
        return pltpu.make_async_remote_copy(
            src_ref=buf.at[pl.ds(h, rows), :, t], dst_ref=buf.at[pl.ds(h, rows), :, owner],
            send_sem=ssem.at[h, t], recv_sem=rsem.at[h, owner], device_id=(1, t), device_id_type=MESH)

    def z_head(q, t, owner):
        return pltpu.make_async_remote_copy(
            src_ref=buf.at[0, pl.ds(*HEAD[q]), t], dst_ref=buf.at[0, pl.ds(*HEAD[q]), owner],
            send_sem=esem.at[q, t], recv_sem=fsem.at[q, owner], device_id=(1, t), device_id_type=MESH)

    barrier = pltpu.get_barrier_semaphore()

    @pl.when(pp == 0)
    def _():
        for k in range(1, TP):
            pl.semaphore_signal(barrier, inc=1, device_id=(0, lax.rem(tp + k, TP)), device_id_type=MESH)
        for k in range(TP):
            pl.semaphore_signal(barrier, inc=1, device_id=(1, lax.rem(tp + k, TP)), device_id_type=MESH)

    helps = jnp.logical_and(pp == 1, core == 1)
    has_w = jnp.logical_or(pp == 0, helps)

    @pl.when(pp == 0)
    def _():
        vec_copy(0).start()
        vec_copy(1).start()

    @pl.when(has_w)
    def _():
        w_local(0).start()
        w_local(1).start()

    @pl.when(pp == 0)
    def _():
        x_copy(0).start()
        x_copy(1).start()
        for i in range(2):
            vec_copy(i).wait()
            sb[tp, i : i + 1, :] = jnp.concatenate([vecs[i], vecs[i]], axis=1)

    pl.semaphore_wait(barrier, TP - 1 + pp)

    @pl.when(pp == 1)
    def _():
        for k in range(TP):
            pl.semaphore_signal(ready, inc=1, device_id=(0, lax.rem(tp + k, TP)), device_id_type=MESH)

    @pl.when(pp == 0)
    def _():
        for k in range(1, TP):
            b_copy(k, tp).start()

    @pl.when(has_w)
    def _():
        w_local(0).wait()
        w_local(1).wait()

    def w_sends(act_on, stages):
        for part, c in stages:
            sends = jnp.logical_or(jnp.logical_and(pp == 0, core == 0), helps)
            if (part, c) == FIRST[0]:
                sends = pp == 0

            @pl.when(sends)
            def _():
                act_on(w_copy(part, tp, c, far * 2 + c))

            if c == 0:
                @pl.when(pp == 0)
                def _():
                    act_on(w_copy(part, tp, 2, chip * 2 + 1 - core))

    w_sends(lambda c: c.start(), FIRST)

    @pl.when(pp == 1)
    def _():
        w_sends(lambda c: c.start(), REST)

    @pl.when(pp == 0)
    def _():
        def start_x(h, _):
            x_copy(h).start()
            return 0
        lax.fori_loop(2, H, start_x, 0)

        zero = jnp.zeros((W + 2, N_LOC, C), jnp.bfloat16)
        xpad[0] = zero
        xpad[H + 1] = zero
        xpad[:, 0] = zero
        xpad[:, W + 1] = zero

        for k in range(1, TP):
            b_copy(k, lax.rem(tp + k, TP)).wait_recv()

        low = lax.broadcasted_iota(jnp.int32, (1, LANES), 1) < CB

        def wait_w(part):
            for k in range(1, TP):
                w_copy(part, lax.rem(tp + k, TP), 0, tp).wait_recv()

        def pixels(h, half, start, count, first_tap):
            sc = jnp.where(low, sb[2 * half, 0:1, :], sb[2 * half + 1, 0:1, :])
            sh = jnp.where(low, sb[2 * half, 1:2, :], sb[2 * half + 1, 1:2, :])

            def conv(w0):
                acc = None
                for tap in range(first_tap, 9):
                    lhs = xpad[h + tap // 3, pl.ds(w0 + tap % 3, count)].reshape(count * N_LOC, C)
                    part = jnp.dot(lhs, wf[half, tap].reshape(C, LANES), preferred_element_type=jnp.float32)
                    acc = part if acc is None else acc + part
                return jnp.maximum(acc * sc + sh, 0.0)

            even, odd = conv(start), conv(PAIRS + start)
            first = jnp.where(low, even, pltpu.roll(odd, CB, 1)).astype(jnp.bfloat16)
            second = jnp.where(low, pltpu.roll(even, CB, 1), odd).astype(jnp.bfloat16)
            buf[h, pl.ds(start, count), 2 * half] = first.reshape(count, N_LOC, LANES)
            buf[h, pl.ds(start, count), 2 * half + 1] = second.reshape(count, N_LOC, LANES)

        x_copy(0).wait()
        x_copy(1).wait()
        wait_w(0)
        wait_w(1)
        for q, (start, count) in enumerate(HEAD):
            pixels(0, chip, start, count, 3)
            if q == 0:
                pl.semaphore_wait(ready, TP)
            for k in ORDER:
                z_head(q, 2 * chip + k, tp).start()
        w_sends(lambda c: c.start(), REST)
        wait_w(2)

        def step(i, _):
            g, r = i // (2 * G), i % (2 * G)
            own = r < G
            half = jnp.where(own, chip, far)
            h = g * G + r % G

            @pl.when(i == G)
            def _():
                wait_w(3)

            @pl.when(jnp.logical_and(own, h < LAST))
            def _():
                x_copy(h + 1).wait()

            for q in range(2):
                pixels(h, half, q * Q, Q, 0)

            def send(first, rows, cores):
                for k in cores:
                    z_copy(first, rows, 2 * half + k, tp).start()

            @pl.when(h == 0)
            def _():
                send(0, 1, (0, 1))

            for first, rows in ROWS[:-1]:
                @pl.when(h == first + rows - 1)
                def _():
                    send(first, rows, (0, 1))

            last = jnp.logical_and(own, core == LATER)

            @pl.when(h == SPLIT - 1)
            def _():
                send(*ROWS[-1], (SOON,))

            @pl.when(jnp.logical_and(h == SPLIT - 1, jnp.logical_not(last)))
            def _():
                send(*ROWS[-1], (LATER,))

            @pl.when(jnp.logical_and(h == LATER_SPLIT - 1, core == LATER))
            def _():
                send(*LATER_ROWS, (SOON,))

            @pl.when(jnp.logical_and(h == LATER_SPLIT - 1, last))
            def _():
                send(*ROWS[-1], (LATER,))

            @pl.when(jnp.logical_and(h == LATER_SPLIT - 1, core == LATER))
            def _():
                send(*LATER_ROWS, (LATER,))
            return 0
        lax.fori_loop(1, 2 * H, step, 0)

        def clear(h, _):
            out[h] = jnp.zeros((W, CB, LANES), jnp.bfloat16)
            return 0
        lax.fori_loop(0, SPLIT, clear, 0)

        for k in range(1, TP):
            b_copy(k, tp).wait_send()

    w_sends(lambda c: c.wait_send(), FIRST + REST)

    @pl.when(pp == 0)
    def _():
        for k in range(2):
            for q in range(len(HEAD)):
                z_head(q, 2 * chip + k, tp).wait_send()
            z_copy(0, 1, 2 * far + k, tp).wait_send()
        for t in range(TP):
            for first, rows in ROWS:
                z_copy(first, rows, t, tp).wait_send()

            @pl.when(core == LATER)
            def _():
                z_copy(*LATER_ROWS, t, tp).wait_send()

    @pl.when(pp == 1)
    def _():
        def turn_rows(first, rows):
            def row(h, _):
                for p in range(PAIRS):
                    turn(buf[h, p].reshape(LANES, LANES), out, h, p)
                return 0
            lax.fori_loop(first, first + rows, row, 0)

        for k in range(2):
            for q in range(len(HEAD)):
                z_head(q, 2 * chip + k, 2 * chip + k).wait_recv()
            z_copy(0, 1, 2 * far + k, 2 * far + k).wait_recv()
        turn_rows(0, 1)
        for first, rows in ROWS:
            for s in range(TP):
                z_copy(first, rows, s, s).wait_recv()
            turn_rows(first, rows)
        for s in (LATER, 2 + LATER):
            z_copy(*LATER_ROWS, s, s).wait_recv()


def turn(block, out, h, p):
    turned = block.T
    out[h, p] = turned[:CB]
    out[h, p + PAIRS] = turned[CB:]


def finish(z, _, out, got, ssem, rsem, tsem, usem, ready):
    pp, tp = lax.axis_index("pp"), lax.axis_index("tp")
    core = tp % 2
    source = pp == 0
    soon = core == SOON

    def z_copy(first, rows, t, owner):
        return pltpu.make_async_remote_copy(
            src_ref=z.at[pl.ds(SPLIT + first, rows), :, t], dst_ref=got.at[pl.ds(first, rows), :, owner],
            send_sem=ssem.at[first, t], recv_sem=rsem.at[first, owner], device_id=(1, t), device_id_type=MESH)

    def z_tail(q, t, owner):
        return pltpu.make_async_remote_copy(
            src_ref=z.at[LAST, pl.ds(*TAIL[q]), t], dst_ref=got.at[LATE - 1, pl.ds(*TAIL[q]), owner],
            send_sem=tsem.at[q, t], recv_sem=usem.at[q, owner], device_id=(1, t), device_id_type=MESH)

    def copies(rows, t, owner):
        return [z_copy(*r, t, owner) for r in rows] + [z_tail(q, t, owner) for q in range(len(TAIL))]

    barrier = pltpu.get_barrier_semaphore()

    def greet(where, targets):
        @pl.when(where)
        def _():
            for target in targets:
                pl.semaphore_signal(barrier, inc=1, device_id=target, device_id_type=MESH)

    greet(source & soon, [(1, 0), (1, 1), (1, 2), (1, 3), (0, lax.rem(tp + 2, TP))])
    greet(source & ~soon, [(1, LATER), (1, 2 + LATER)])
    greet(~source & soon, [(0, LATER), (0, 2 + LATER)])
    pl.semaphore_wait(barrier, jnp.where(source, jnp.where(soon, 1, 2), jnp.where(soon, 2, 4)))

    @pl.when(~source & soon)
    def _():
        for t in (SOON, 2 + SOON):
            pl.semaphore_signal(ready.at[0], inc=1, device_id=(0, t), device_id_type=MESH)

    @pl.when(~source & ~soon)
    def _():
        for t in range(TP):
            pl.semaphore_signal(ready.at[1], inc=1, device_id=(0, t), device_id_type=MESH)

    def sends(rows, k):
        for a in zip(*[copies(rows, t, tp) for t in (k, 2 + k)]):
            for c in a:
                c.start()

    chip, far = tp // 2, 1 - tp // 2

    @pl.when(source & soon)
    def _():
        pl.semaphore_wait(ready.at[0], 2)
        for c in copies(LATE_SOON, 2 * chip + SOON, tp):
            c.start()
        z_copy(*LATE_SOON[0], 2 * chip + SOON, tp).wait_send()
        for c in copies(LATE_SOON, 2 * far + SOON, tp):
            c.start()
        pl.semaphore_wait(ready.at[1], 2)
        sends(LATE_SOON, LATER)

    @pl.when(source & ~soon)
    def _():
        sends(LATE_LATER, SOON)
        pl.semaphore_wait(ready.at[1], 2)
        sends(LATE_LATER, LATER)

    @pl.when(source)
    def _():
        def clear(h, _):
            out[h] = jnp.zeros((W, CB, LANES), jnp.bfloat16)
            return 0
        lax.fori_loop(0, LATE, clear, 0)
        for rows, where in ((LATE_SOON, soon), (LATE_LATER, ~soon)):
            @pl.when(where)
            def _():
                for c in copies(rows[1:] if where is soon else rows, 2 * chip + SOON, tp):
                    c.wait_send()
                for t in (2 * chip + LATER, 2 * far, 2 * far + 1):
                    for c in copies(rows, t, tp):
                        c.wait_send()

    @pl.when(~source)
    def _():
        for s in (SOON, 2 + SOON):
            for piece in LATE_SOON:
                z_copy(*piece, s, s).wait_recv()

        def mixed(h, _):
            for p in range(PAIRS):
                parts = [got[h, p, s] if s % 2 == SOON else z[SPLIT + h, p, s] for s in range(TP)]
                turn(jnp.concatenate(parts, axis=0), out, h, p)
            return 0
        lax.fori_loop(0, LATER_SPLIT - SPLIT, mixed, 0)
        for first, rows in LATE_LATER:
            for s in range(TP):
                z_copy(first, rows, s, s).wait_recv()

            def row(h, _):
                for p in range(PAIRS):
                    turn(got[h, p].reshape(LANES, LANES), out, h, p)
                return 0
            lax.fori_loop(first, first + rows, row, 0)
        for q, (start, count) in enumerate(TAIL):
            for s in range(TP):
                z_tail(q, s, s).wait_recv()
            for p in range(start, start + count):
                turn(got[LATE - 1, p].reshape(LANES, LANES), out, LATE - 1, p)


def write(first, rows, each, src, *refs):
    dst, _, sem = refs[-3:]
    copies = [pltpu.make_async_copy(src.at[pl.ds(i * each, each)], dst.at[pl.ds(first + i * each, each)], sem.at[i])
              for i in range(rows // each)]
    for c in copies:
        c.start()
    for c in copies:
        c.wait()


def solution(mesh):
    def local_step(act, w, scale, shift):
        x = jnp.transpose(act, (1, 2, 0, 3))
        dma = pltpu.SemaphoreType.DMA
        shape = (H, W, CB, LANES)
        vmem, hbm = pl.BlockSpec(memory_space=pltpu.VMEM), pl.BlockSpec(memory_space=pl.ANY)
        early, z = pl.pallas_call(
            kernel,
            out_shape=(pltpu.VMEM((SPLIT, W, CB, LANES), jnp.bfloat16),
                       pltpu.VMEM((H, PAIRS, TP, N_LOC, LANES), jnp.bfloat16)),
            in_specs=[pl.BlockSpec(memory_space=pl.ANY), pl.BlockSpec(memory_space=pl.ANY),
                      pl.BlockSpec(memory_space=pl.ANY), pl.BlockSpec(memory_space=pl.ANY)],
            out_specs=(vmem, vmem),
            scratch_shapes=[
                pltpu.VMEM((H + 2, W + 2, N_LOC, C), jnp.bfloat16),
                pltpu.VMEM((2, 9, TP, C // TP, LANES), jnp.bfloat16),
                pltpu.VMEM((TP, 8, LANES), jnp.float32),
                dma((H,)), dma((2,)), dma((4, 3)), dma((4, TP)), dma((TP,)), dma((TP,)), dma((H, TP)), dma((H, TP)),
                dma((2, TP)), dma((2, TP)), pltpu.VMEM((2, 1, CB), jnp.float32), dma((2,)), pltpu.SemaphoreType.REGULAR,
            ],
            compiler_params=pltpu.CompilerParams(collective_id=0, has_side_effects=True, vmem_limit_bytes=42677043),
        )(x, w.reshape(9, C // TP, C), scale.reshape(1, CB), shift.reshape(1, CB))
        small = pltpu.CompilerParams(vmem_limit_bytes=2**20)
        written = (jax.ShapeDtypeStruct(shape, jnp.bfloat16), jax.ShapeDtypeStruct((8, LANES), jnp.float32))
        out, token = pl.pallas_call(
            functools.partial(write, 0, SPLIT, 1), out_shape=written, in_specs=[vmem], out_specs=(hbm, hbm), scratch_shapes=[dma((SPLIT // 1,))], compiler_params=small)(early)
        late = pl.pallas_call(
            finish,
            out_shape=pltpu.VMEM((LATE, W, CB, LANES), jnp.bfloat16),
            in_specs=[vmem, hbm],
            out_specs=vmem,
            scratch_shapes=[
                pltpu.VMEM((LATE, PAIRS, TP, N_LOC, LANES), jnp.bfloat16),
                dma((LATE, TP)), dma((LATE, TP)), dma((2, TP)), dma((2, TP)), pltpu.SemaphoreType.REGULAR((2,)),
            ],
            compiler_params=pltpu.CompilerParams(collective_id=1, has_side_effects=True, vmem_limit_bytes=12 * 2**20),
        )(z, token)
        out, _ = pl.pallas_call(
            functools.partial(write, SPLIT, LATE, 1), out_shape=written, in_specs=[vmem, hbm], out_specs=(hbm, hbm), scratch_shapes=[dma((LATE // 1,))], input_output_aliases={1: 0}, compiler_params=small)(late, out)
        return jnp.transpose(out, (3, 0, 1, 2))

    return jax.shard_map(local_step, mesh=mesh, in_specs=(P(("pp", "tp")), P(None, None, "tp", None), P("tp"), P("tp")),
                         out_specs=P("pp", None, None, "tp"), check_vma=False)
```

```python
import functools

import jax
import jax.numpy as jnp
from jax import lax
from jax.experimental import pallas as pl
from jax.experimental.pallas import tpu as pltpu
from jax.sharding import PartitionSpec as P

MESH = pl.DeviceIdType.MESH
H, W, C = 28, 28, 256
N_LOC = 32
TP = 4
CB = C // TP
LANES = 128
PAIRS = W // 2
Q = 7
G = 4
GROUPS = H // G
LAST = H - 1
SOON, LATER = 1, 0
SPLIT = 23
LATER_SPLIT = 27
LATE = H - SPLIT
PARTS = ((0, 3, 3), (0, 6, 3), (0, 0, 3), (1, 0, 9))
ORDER = (1, 0)
FIRST = ((0, 0), (1, 0), (0, 1), (1, 1))
REST = ((2, 0), (2, 1), (3, 0), (3, 1))
HEAD = ((0, 2), (2, 12))
ROWS = ((1, 1), (2, 6), (8, 15))
LATER_ROWS = (SPLIT, LATER_SPLIT - SPLIT)
LATE_SOON = ((0, 2), (2, 2))
LATE_LATER = ()
TAIL = ((0, 12), (12, 2))


def kernel(act, w, scale, shift, out, buf, xpad, wf, sb, xsem, wlsem, wssem, wrsem, bssem, brsem, ssem, rsem, esem, fsem, vecs, vsem, ready):
    pp, tp = lax.axis_index("pp"), lax.axis_index("tp")
    chip, core = tp // 2, tp % 2
    far = 1 - chip

    def half_of(sel, receiver):
        return receiver if sel == 0 else 1 - receiver

    def w_local(half):
        return pltpu.make_async_copy(
            w.at[:, :, pl.ds(pl.multiple_of(half * LANES, LANES), LANES)], wf.at[half, :, tp], wlsem.at[half])

    def w_copy(part, owner, slot, target):
        sel, tap, taps = PARTS[part]
        block = wf.at[half_of(sel, target // 2), pl.ds(tap, taps), owner]
        return pltpu.make_async_remote_copy(
            src_ref=block, dst_ref=block, send_sem=wssem.at[part, slot], recv_sem=wrsem.at[part, owner],
            device_id=(0, target), device_id_type=MESH)

    def x_copy(h):
        return pltpu.make_async_copy(act.at[h], xpad.at[h + 1, pl.ds(1, W)], xsem.at[h])

    def vec_copy(i):
        return pltpu.make_async_copy((scale, shift)[i], vecs.at[i], vsem.at[i])

    def b_copy(k, owner):
        return pltpu.make_async_remote_copy(
            src_ref=sb.at[tp], dst_ref=sb.at[tp], send_sem=bssem.at[k], recv_sem=brsem.at[owner],
            device_id=(0, lax.rem(tp + k, TP)), device_id_type=MESH)

    def z_copy(h, rows, t, owner):
        return pltpu.make_async_remote_copy(
            src_ref=buf.at[pl.ds(h, rows), :, t], dst_ref=buf.at[pl.ds(h, rows), :, owner],
            send_sem=ssem.at[h, t], recv_sem=rsem.at[h, owner], device_id=(1, t), device_id_type=MESH)

    def z_head(q, t, owner):
        return pltpu.make_async_remote_copy(
            src_ref=buf.at[0, pl.ds(*HEAD[q]), t], dst_ref=buf.at[0, pl.ds(*HEAD[q]), owner],
            send_sem=esem.at[q, t], recv_sem=fsem.at[q, owner], device_id=(1, t), device_id_type=MESH)

    barrier = pltpu.get_barrier_semaphore()

    @pl.when(pp == 0)
    def _():
        for k in range(1, TP):
            pl.semaphore_signal(barrier, inc=1, device_id=(0, lax.rem(tp + k, TP)), device_id_type=MESH)
        for k in range(TP):
            pl.semaphore_signal(barrier, inc=1, device_id=(1, lax.rem(tp + k, TP)), device_id_type=MESH)

    helps = jnp.logical_and(pp == 1, core == 1)
    has_w = jnp.logical_or(pp == 0, helps)

    @pl.when(pp == 0)
    def _():
        vec_copy(0).start()
        vec_copy(1).start()

    @pl.when(has_w)
    def _():
        w_local(0).start()
        w_local(1).start()

    @pl.when(pp == 0)
    def _():
        x_copy(0).start()
        x_copy(1).start()
        for i in range(2):
            vec_copy(i).wait()
            sb[tp, i : i + 1, :] = jnp.concatenate([vecs[i], vecs[i]], axis=1)

    pl.semaphore_wait(barrier, TP - 1 + pp)

    @pl.when(pp == 1)
    def _():
        for k in range(TP):
            pl.semaphore_signal(ready, inc=1, device_id=(0, lax.rem(tp + k, TP)), device_id_type=MESH)

    @pl.when(pp == 0)
    def _():
        for k in range(1, TP):
            b_copy(k, tp).start()

    @pl.when(has_w)
    def _():
        w_local(0).wait()
        w_local(1).wait()

    def w_sends(act_on, stages):
        for part, c in stages:
            sends = jnp.logical_or(jnp.logical_and(pp == 0, core == 0), helps)
            if (part, c) == FIRST[0]:
                sends = pp == 0

            @pl.when(sends)
            def _():
                act_on(w_copy(part, tp, c, far * 2 + c))

            if c == 0:
                @pl.when(pp == 0)
                def _():
                    act_on(w_copy(part, tp, 2, chip * 2 + 1 - core))

    w_sends(lambda c: c.start(), FIRST)

    @pl.when(pp == 1)
    def _():
        w_sends(lambda c: c.start(), REST)

    @pl.when(pp == 0)
    def _():
        def start_x(h, _):
            x_copy(h).start()
            return 0
        lax.fori_loop(2, H, start_x, 0)

        zero = jnp.zeros((W + 2, N_LOC, C), jnp.bfloat16)
        xpad[0] = zero
        xpad[H + 1] = zero
        xpad[:, 0] = zero
        xpad[:, W + 1] = zero

        for k in range(1, TP):
            b_copy(k, lax.rem(tp + k, TP)).wait_recv()

        low = lax.broadcasted_iota(jnp.int32, (1, LANES), 1) < CB

        def wait_w(part):
            for k in range(1, TP):
                w_copy(part, lax.rem(tp + k, TP), 0, tp).wait_recv()

        def pixels(h, half, start, count, first_tap):
            sc = jnp.where(low, sb[2 * half, 0:1, :], sb[2 * half + 1, 0:1, :])
            sh = jnp.where(low, sb[2 * half, 1:2, :], sb[2 * half + 1, 1:2, :])

            def conv(w0):
                acc = None
                for tap in range(first_tap, 9):
                    lhs = xpad[h + tap // 3, pl.ds(w0 + tap % 3, count)].reshape(count * N_LOC, C)
                    part = jnp.dot(lhs, wf[half, tap].reshape(C, LANES), preferred_element_type=jnp.float32)
                    acc = part if acc is None else acc + part
                return jnp.maximum(acc * sc + sh, 0.0)

            even, odd = conv(start), conv(PAIRS + start)
            first = jnp.where(low, even, pltpu.roll(odd, CB, 1)).astype(jnp.bfloat16)
            second = jnp.where(low, pltpu.roll(even, CB, 1), odd).astype(jnp.bfloat16)
            buf[h, pl.ds(start, count), 2 * half] = first.reshape(count, N_LOC, LANES)
            buf[h, pl.ds(start, count), 2 * half + 1] = second.reshape(count, N_LOC, LANES)

        x_copy(0).wait()
        x_copy(1).wait()
        wait_w(0)
        wait_w(1)
        for q, (start, count) in enumerate(HEAD):
            pixels(0, chip, start, count, 3)
            if q == 0:
                pl.semaphore_wait(ready, TP)
            for k in ORDER:
                z_head(q, 2 * chip + k, tp).start()
        w_sends(lambda c: c.start(), REST)
        wait_w(2)

        def step(i, _):
            g, r = i // (2 * G), i % (2 * G)
            own = r < G
            half = jnp.where(own, chip, far)
            h = g * G + r % G

            @pl.when(i == G)
            def _():
                wait_w(3)

            @pl.when(jnp.logical_and(own, h < LAST))
            def _():
                x_copy(h + 1).wait()

            for q in range(2):
                pixels(h, half, q * Q, Q, 0)

            def send(first, rows, cores):
                for k in cores:
                    z_copy(first, rows, 2 * half + k, tp).start()

            @pl.when(h == 0)
            def _():
                send(0, 1, (0, 1))

            for first, rows in ROWS[:-1]:
                @pl.when(h == first + rows - 1)
                def _():
                    send(first, rows, (0, 1))

            last = jnp.logical_and(own, core == LATER)

            @pl.when(h == SPLIT - 1)
            def _():
                send(*ROWS[-1], (SOON,))

            @pl.when(jnp.logical_and(h == SPLIT - 1, jnp.logical_not(last)))
            def _():
                send(*ROWS[-1], (LATER,))

            @pl.when(jnp.logical_and(h == LATER_SPLIT - 1, core == LATER))
            def _():
                send(*LATER_ROWS, (SOON,))

            @pl.when(jnp.logical_and(h == LATER_SPLIT - 1, last))
            def _():
                send(*ROWS[-1], (LATER,))

            @pl.when(jnp.logical_and(h == LATER_SPLIT - 1, core == LATER))
            def _():
                send(*LATER_ROWS, (LATER,))
            return 0
        lax.fori_loop(1, 2 * H, step, 0)

        def clear(h, _):
            out[h] = jnp.zeros((W, CB, LANES), jnp.bfloat16)
            return 0
        lax.fori_loop(0, SPLIT, clear, 0)

        for k in range(1, TP):
            b_copy(k, tp).wait_send()

    w_sends(lambda c: c.wait_send(), FIRST + REST)

    @pl.when(pp == 0)
    def _():
        for k in range(2):
            for q in range(len(HEAD)):
                z_head(q, 2 * chip + k, tp).wait_send()
            z_copy(0, 1, 2 * far + k, tp).wait_send()
        for t in range(TP):
            for first, rows in ROWS:
                z_copy(first, rows, t, tp).wait_send()

            @pl.when(core == LATER)
            def _():
                z_copy(*LATER_ROWS, t, tp).wait_send()

    @pl.when(pp == 1)
    def _():
        def turn_rows(first, rows):
            def row(h, _):
                for p in range(PAIRS):
                    turn(buf[h, p].reshape(LANES, LANES), out, h, p)
                return 0
            lax.fori_loop(first, first + rows, row, 0)

        for k in range(2):
            for q in range(len(HEAD)):
                z_head(q, 2 * chip + k, 2 * chip + k).wait_recv()
            z_copy(0, 1, 2 * far + k, 2 * far + k).wait_recv()
        turn_rows(0, 1)
        for first, rows in ROWS:
            for s in range(TP):
                z_copy(first, rows, s, s).wait_recv()
            turn_rows(first, rows)
        for s in (LATER, 2 + LATER):
            z_copy(*LATER_ROWS, s, s).wait_recv()


def turn(block, out, h, p):
    turned = block.T
    out[h, p] = turned[:CB]
    out[h, p + PAIRS] = turned[CB:]


def finish(z, _, out, got, ssem, rsem, tsem, usem, ready):
    pp, tp = lax.axis_index("pp"), lax.axis_index("tp")
    core = tp % 2
    source = pp == 0
    soon = core == SOON

    def z_copy(first, rows, t, owner):
        return pltpu.make_async_remote_copy(
            src_ref=z.at[pl.ds(SPLIT + first, rows), :, t], dst_ref=got.at[pl.ds(first, rows), :, owner],
            send_sem=ssem.at[first, t], recv_sem=rsem.at[first, owner], device_id=(1, t), device_id_type=MESH)

    def z_tail(q, t, owner):
        return pltpu.make_async_remote_copy(
            src_ref=z.at[LAST, pl.ds(*TAIL[q]), t], dst_ref=got.at[LATE - 1, pl.ds(*TAIL[q]), owner],
            send_sem=tsem.at[q, t], recv_sem=usem.at[q, owner], device_id=(1, t), device_id_type=MESH)

    def copies(rows, t, owner):
        return [z_copy(*r, t, owner) for r in rows] + [z_tail(q, t, owner) for q in range(len(TAIL))]

    barrier = pltpu.get_barrier_semaphore()

    def greet(where, targets):
        @pl.when(where)
        def _():
            for target in targets:
                pl.semaphore_signal(barrier, inc=1, device_id=target, device_id_type=MESH)

    greet(source & soon, [(1, 0), (1, 1), (1, 2), (1, 3), (0, lax.rem(tp + 2, TP))])
    greet(source & ~soon, [(1, LATER), (1, 2 + LATER)])
    greet(~source & soon, [(0, LATER), (0, 2 + LATER)])
    pl.semaphore_wait(barrier, jnp.where(source, jnp.where(soon, 1, 2), jnp.where(soon, 2, 4)))

    @pl.when(~source & soon)
    def _():
        for t in (SOON, 2 + SOON):
            pl.semaphore_signal(ready.at[0], inc=1, device_id=(0, t), device_id_type=MESH)

    @pl.when(~source & ~soon)
    def _():
        for t in range(TP):
            pl.semaphore_signal(ready.at[1], inc=1, device_id=(0, t), device_id_type=MESH)

    def sends(rows, k):
        for a in zip(*[copies(rows, t, tp) for t in (k, 2 + k)]):
            for c in a:
                c.start()

    chip, far = tp // 2, 1 - tp // 2

    @pl.when(source & soon)
    def _():
        pl.semaphore_wait(ready.at[0], 2)
        for c in copies(LATE_SOON, 2 * chip + SOON, tp):
            c.start()
        z_copy(*LATE_SOON[0], 2 * chip + SOON, tp).wait_send()
        for c in copies(LATE_SOON, 2 * far + SOON, tp):
            c.start()
        pl.semaphore_wait(ready.at[1], 2)
        sends(LATE_SOON, LATER)

    @pl.when(source & ~soon)
    def _():
        sends(LATE_LATER, SOON)
        pl.semaphore_wait(ready.at[1], 2)
        sends(LATE_LATER, LATER)

    @pl.when(source)
    def _():
        def clear(h, _):
            out[h] = jnp.zeros((W, CB, LANES), jnp.bfloat16)
            return 0
        lax.fori_loop(0, LATE, clear, 0)
        for rows, where in ((LATE_SOON, soon), (LATE_LATER, ~soon)):
            @pl.when(where)
            def _():
                for c in copies(rows[1:] if where is soon else rows, 2 * chip + SOON, tp):
                    c.wait_send()
                for t in (2 * chip + LATER, 2 * far, 2 * far + 1):
                    for c in copies(rows, t, tp):
                        c.wait_send()

    @pl.when(~source)
    def _():
        for s in (SOON, 2 + SOON):
            for piece in LATE_SOON:
                z_copy(*piece, s, s).wait_recv()

        def mixed(h, _):
            for p in range(PAIRS):
                parts = [got[h, p, s] if s % 2 == SOON else z[SPLIT + h, p, s] for s in range(TP)]
                turn(jnp.concatenate(parts, axis=0), out, h, p)
            return 0
        lax.fori_loop(0, LATER_SPLIT - SPLIT, mixed, 0)
        for first, rows in LATE_LATER:
            for s in range(TP):
                z_copy(first, rows, s, s).wait_recv()

            def row(h, _):
                for p in range(PAIRS):
                    turn(got[h, p].reshape(LANES, LANES), out, h, p)
                return 0
            lax.fori_loop(first, first + rows, row, 0)
        for q, (start, count) in enumerate(TAIL):
            for s in range(TP):
                z_tail(q, s, s).wait_recv()
            for p in range(start, start + count):
                turn(got[LATE - 1, p].reshape(LANES, LANES), out, LATE - 1, p)


def write(first, rows, each, src, *refs):
    dst, _, sem = refs[-3:]
    copies = [pltpu.make_async_copy(src.at[pl.ds(i * each, each)], dst.at[pl.ds(first + i * each, each)], sem.at[i])
              for i in range(rows // each)]
    for c in copies:
        c.start()
    for c in copies:
        c.wait()


def solution(mesh):
    def local_step(act, w, scale, shift):
        x = jnp.transpose(act, (1, 2, 0, 3))
        dma = pltpu.SemaphoreType.DMA
        shape = (H, W, CB, LANES)
        vmem, hbm = pl.BlockSpec(memory_space=pltpu.VMEM), pl.BlockSpec(memory_space=pl.ANY)
        early, z = pl.pallas_call(
            kernel,
            out_shape=(pltpu.VMEM((SPLIT, W, CB, LANES), jnp.bfloat16),
                       pltpu.VMEM((H, PAIRS, TP, N_LOC, LANES), jnp.bfloat16)),
            in_specs=[pl.BlockSpec(memory_space=pl.ANY), pl.BlockSpec(memory_space=pl.ANY),
                      pl.BlockSpec(memory_space=pl.ANY), pl.BlockSpec(memory_space=pl.ANY)],
            out_specs=(vmem, vmem),
            scratch_shapes=[
                pltpu.VMEM((H + 2, W + 2, N_LOC, C), jnp.bfloat16),
                pltpu.VMEM((2, 9, TP, C // TP, LANES), jnp.bfloat16),
                pltpu.VMEM((TP, 8, LANES), jnp.float32),
                dma((H,)), dma((2,)), dma((4, 3)), dma((4, TP)), dma((TP,)), dma((TP,)), dma((H, TP)), dma((H, TP)),
                dma((2, TP)), dma((2, TP)), pltpu.VMEM((2, 1, CB), jnp.float32), dma((2,)), pltpu.SemaphoreType.REGULAR,
            ],
            compiler_params=pltpu.CompilerParams(collective_id=0, has_side_effects=True, vmem_limit_bytes=42677043),
        )(x, w.reshape(9, C // TP, C), scale.reshape(1, CB), shift.reshape(1, CB))
        small = pltpu.CompilerParams(vmem_limit_bytes=2**20)
        written = (jax.ShapeDtypeStruct(shape, jnp.bfloat16), jax.ShapeDtypeStruct((8, LANES), jnp.float32))
        out, token = pl.pallas_call(
            functools.partial(write, 0, SPLIT, 1), out_shape=written, in_specs=[vmem], out_specs=(hbm, hbm), scratch_shapes=[dma((SPLIT // 1,))], compiler_params=small)(early)
        late = pl.pallas_call(
            finish,
            out_shape=pltpu.VMEM((LATE, W, CB, LANES), jnp.bfloat16),
            in_specs=[vmem, hbm],
            out_specs=vmem,
            scratch_shapes=[
                pltpu.VMEM((LATE, PAIRS, TP, N_LOC, LANES), jnp.bfloat16),
                dma((LATE, TP)), dma((LATE, TP)), dma((2, TP)), dma((2, TP)), pltpu.SemaphoreType.REGULAR((2,)),
            ],
            compiler_params=pltpu.CompilerParams(collective_id=1, has_side_effects=True, vmem_limit_bytes=12 * 2**20),
        )(z, token)
        out, _ = pl.pallas_call(
            functools.partial(write, SPLIT, LATE, 5), out_shape=written, in_specs=[vmem, hbm], out_specs=(hbm, hbm), scratch_shapes=[dma((LATE // 5,))], input_output_aliases={1: 0}, compiler_params=small)(late, out)
        return jnp.transpose(out, (3, 0, 1, 2))

    return jax.shard_map(local_step, mesh=mesh, in_specs=(P(("pp", "tp")), P(None, None, "tp", None), P("tp"), P("tp")),
                         out_specs=P("pp", None, None, "tp"), check_vma=False)
```

```python
import functools

import jax
import jax.numpy as jnp
from jax import lax
from jax.experimental import pallas as pl
from jax.experimental.pallas import tpu as pltpu
from jax.sharding import PartitionSpec as P

MESH = pl.DeviceIdType.MESH
H, W, C = 28, 28, 256
N_LOC = 32
TP = 4
CB = C // TP
LANES = 128
PAIRS = W // 2
Q = 7
G = 4
GROUPS = H // G
LAST = H - 1
SOON, LATER = 1, 0
SPLIT = 23
LATER_SPLIT = 27
LATE = H - SPLIT
PARTS = ((0, 3, 3), (0, 6, 3), (0, 0, 3), (1, 0, 9))
ORDER = (1, 0)
FIRST = ((0, 0), (1, 0), (0, 1), (1, 1))
REST = ((2, 0), (2, 1), (3, 0), (3, 1))
HEAD = ((0, 3), (3, 11))
ROWS = ((1, 1), (2, 6), (8, 15))
LATER_ROWS = (SPLIT, LATER_SPLIT - SPLIT)
LATE_SOON = ((0, 2), (2, 2))
LATE_LATER = ()
TAIL = ((0, 12), (12, 2))


def kernel(act, w, scale, shift, out, buf, xpad, wf, sb, xsem, wlsem, wssem, wrsem, bssem, brsem, ssem, rsem, esem, fsem, vecs, vsem, ready):
    pp, tp = lax.axis_index("pp"), lax.axis_index("tp")
    chip, core = tp // 2, tp % 2
    far = 1 - chip

    def half_of(sel, receiver):
        return receiver if sel == 0 else 1 - receiver

    def w_local(half):
        return pltpu.make_async_copy(
            w.at[:, :, pl.ds(pl.multiple_of(half * LANES, LANES), LANES)], wf.at[half, :, tp], wlsem.at[half])

    def w_copy(part, owner, slot, target):
        sel, tap, taps = PARTS[part]
        block = wf.at[half_of(sel, target // 2), pl.ds(tap, taps), owner]
        return pltpu.make_async_remote_copy(
            src_ref=block, dst_ref=block, send_sem=wssem.at[part, slot], recv_sem=wrsem.at[part, owner],
            device_id=(0, target), device_id_type=MESH)

    def x_copy(h):
        return pltpu.make_async_copy(act.at[h], xpad.at[h + 1, pl.ds(1, W)], xsem.at[h])

    def vec_copy(i):
        return pltpu.make_async_copy((scale, shift)[i], vecs.at[i], vsem.at[i])

    def b_copy(k, owner):
        return pltpu.make_async_remote_copy(
            src_ref=sb.at[tp], dst_ref=sb.at[tp], send_sem=bssem.at[k], recv_sem=brsem.at[owner],
            device_id=(0, lax.rem(tp + k, TP)), device_id_type=MESH)

    def z_copy(h, rows, t, owner):
        return pltpu.make_async_remote_copy(
            src_ref=buf.at[pl.ds(h, rows), :, t], dst_ref=buf.at[pl.ds(h, rows), :, owner],
            send_sem=ssem.at[h, t], recv_sem=rsem.at[h, owner], device_id=(1, t), device_id_type=MESH)

    def z_head(q, t, owner):
        return pltpu.make_async_remote_copy(
            src_ref=buf.at[0, pl.ds(*HEAD[q]), t], dst_ref=buf.at[0, pl.ds(*HEAD[q]), owner],
            send_sem=esem.at[q, t], recv_sem=fsem.at[q, owner], device_id=(1, t), device_id_type=MESH)

    barrier = pltpu.get_barrier_semaphore()

    @pl.when(pp == 0)
    def _():
        for k in range(1, TP):
            pl.semaphore_signal(barrier, inc=1, device_id=(0, lax.rem(tp + k, TP)), device_id_type=MESH)
        for k in range(TP):
            pl.semaphore_signal(barrier, inc=1, device_id=(1, lax.rem(tp + k, TP)), device_id_type=MESH)

    helps = jnp.logical_and(pp == 1, core == 1)
    has_w = jnp.logical_or(pp == 0, helps)

    @pl.when(pp == 0)
    def _():
        vec_copy(0).start()
        vec_copy(1).start()

    @pl.when(has_w)
    def _():
        w_local(0).start()
        w_local(1).start()

    @pl.when(pp == 0)
    def _():
        x_copy(0).start()
        x_copy(1).start()
        for i in range(2):
            vec_copy(i).wait()
            sb[tp, i : i + 1, :] = jnp.concatenate([vecs[i], vecs[i]], axis=1)

    pl.semaphore_wait(barrier, TP - 1 + pp)

    @pl.when(pp == 1)
    def _():
        for k in range(TP):
            pl.semaphore_signal(ready, inc=1, device_id=(0, lax.rem(tp + k, TP)), device_id_type=MESH)

    @pl.when(pp == 0)
    def _():
        for k in range(1, TP):
            b_copy(k, tp).start()

    @pl.when(has_w)
    def _():
        w_local(0).wait()
        w_local(1).wait()

    def w_sends(act_on, stages):
        for part, c in stages:
            sends = jnp.logical_or(jnp.logical_and(pp == 0, core == 0), helps)
            if (part, c) == FIRST[0]:
                sends = pp == 0

            @pl.when(sends)
            def _():
                act_on(w_copy(part, tp, c, far * 2 + c))

            if c == 0:
                @pl.when(pp == 0)
                def _():
                    act_on(w_copy(part, tp, 2, chip * 2 + 1 - core))

    w_sends(lambda c: c.start(), FIRST)

    @pl.when(pp == 1)
    def _():
        w_sends(lambda c: c.start(), REST)

    @pl.when(pp == 0)
    def _():
        def start_x(h, _):
            x_copy(h).start()
            return 0
        lax.fori_loop(2, H, start_x, 0)

        zero = jnp.zeros((W + 2, N_LOC, C), jnp.bfloat16)
        xpad[0] = zero
        xpad[H + 1] = zero
        xpad[:, 0] = zero
        xpad[:, W + 1] = zero

        for k in range(1, TP):
            b_copy(k, lax.rem(tp + k, TP)).wait_recv()

        low = lax.broadcasted_iota(jnp.int32, (1, LANES), 1) < CB

        def wait_w(part):
            for k in range(1, TP):
                w_copy(part, lax.rem(tp + k, TP), 0, tp).wait_recv()

        def pixels(h, half, start, count, first_tap):
            sc = jnp.where(low, sb[2 * half, 0:1, :], sb[2 * half + 1, 0:1, :])
            sh = jnp.where(low, sb[2 * half, 1:2, :], sb[2 * half + 1, 1:2, :])

            def conv(w0):
                acc = None
                for tap in range(first_tap, 9):
                    lhs = xpad[h + tap // 3, pl.ds(w0 + tap % 3, count)].reshape(count * N_LOC, C)
                    part = jnp.dot(lhs, wf[half, tap].reshape(C, LANES), preferred_element_type=jnp.float32)
                    acc = part if acc is None else acc + part
                return jnp.maximum(acc * sc + sh, 0.0)

            even, odd = conv(start), conv(PAIRS + start)
            first = jnp.where(low, even, pltpu.roll(odd, CB, 1)).astype(jnp.bfloat16)
            second = jnp.where(low, pltpu.roll(even, CB, 1), odd).astype(jnp.bfloat16)
            buf[h, pl.ds(start, count), 2 * half] = first.reshape(count, N_LOC, LANES)
            buf[h, pl.ds(start, count), 2 * half + 1] = second.reshape(count, N_LOC, LANES)

        x_copy(0).wait()
        x_copy(1).wait()
        wait_w(0)
        wait_w(1)
        for q, (start, count) in enumerate(HEAD):
            pixels(0, chip, start, count, 3)
            if q == 0:
                pl.semaphore_wait(ready, TP)
            for k in ORDER:
                z_head(q, 2 * chip + k, tp).start()
        w_sends(lambda c: c.start(), REST)
        wait_w(2)

        def step(i, _):
            g, r = i // (2 * G), i % (2 * G)
            own = r < G
            half = jnp.where(own, chip, far)
            h = g * G + r % G

            @pl.when(i == G)
            def _():
                wait_w(3)

            @pl.when(jnp.logical_and(own, h < LAST))
            def _():
                x_copy(h + 1).wait()

            for q in range(2):
                pixels(h, half, q * Q, Q, 0)

            def send(first, rows, cores):
                for k in cores:
                    z_copy(first, rows, 2 * half + k, tp).start()

            @pl.when(h == 0)
            def _():
                send(0, 1, (0, 1))

            for first, rows in ROWS[:-1]:
                @pl.when(h == first + rows - 1)
                def _():
                    send(first, rows, (0, 1))

            last = jnp.logical_and(own, core == LATER)

            @pl.when(h == SPLIT - 1)
            def _():
                send(*ROWS[-1], (SOON,))

            @pl.when(jnp.logical_and(h == SPLIT - 1, jnp.logical_not(last)))
            def _():
                send(*ROWS[-1], (LATER,))

            @pl.when(jnp.logical_and(h == LATER_SPLIT - 1, core == LATER))
            def _():
                send(*LATER_ROWS, (SOON,))

            @pl.when(jnp.logical_and(h == LATER_SPLIT - 1, last))
            def _():
                send(*ROWS[-1], (LATER,))

            @pl.when(jnp.logical_and(h == LATER_SPLIT - 1, core == LATER))
            def _():
                send(*LATER_ROWS, (LATER,))
            return 0
        lax.fori_loop(1, 2 * H, step, 0)

        def clear(h, _):
            out[h] = jnp.zeros((W, CB, LANES), jnp.bfloat16)
            return 0
        lax.fori_loop(0, SPLIT, clear, 0)

        for k in range(1, TP):
            b_copy(k, tp).wait_send()

    w_sends(lambda c: c.wait_send(), FIRST + REST)

    @pl.when(pp == 0)
    def _():
        for k in range(2):
            for q in range(len(HEAD)):
                z_head(q, 2 * chip + k, tp).wait_send()
            z_copy(0, 1, 2 * far + k, tp).wait_send()
        for t in range(TP):
            for first, rows in ROWS:
                z_copy(first, rows, t, tp).wait_send()

            @pl.when(core == LATER)
            def _():
                z_copy(*LATER_ROWS, t, tp).wait_send()

    @pl.when(pp == 1)
    def _():
        def turn_rows(first, rows):
            def row(h, _):
                for p in range(PAIRS):
                    turn(buf[h, p].reshape(LANES, LANES), out, h, p)
                return 0
            lax.fori_loop(first, first + rows, row, 0)

        for k in range(2):
            for q in range(len(HEAD)):
                z_head(q, 2 * chip + k, 2 * chip + k).wait_recv()
            z_copy(0, 1, 2 * far + k, 2 * far + k).wait_recv()
        turn_rows(0, 1)
        for first, rows in ROWS:
            for s in range(TP):
                z_copy(first, rows, s, s).wait_recv()
            turn_rows(first, rows)
        for s in (LATER, 2 + LATER):
            z_copy(*LATER_ROWS, s, s).wait_recv()


def turn(block, out, h, p):
    turned = block.T
    out[h, p] = turned[:CB]
    out[h, p + PAIRS] = turned[CB:]


def finish(z, _, out, got, ssem, rsem, tsem, usem, ready):
    pp, tp = lax.axis_index("pp"), lax.axis_index("tp")
    core = tp % 2
    source = pp == 0
    soon = core == SOON

    def z_copy(first, rows, t, owner):
        return pltpu.make_async_remote_copy(
            src_ref=z.at[pl.ds(SPLIT + first, rows), :, t], dst_ref=got.at[pl.ds(first, rows), :, owner],
            send_sem=ssem.at[first, t], recv_sem=rsem.at[first, owner], device_id=(1, t), device_id_type=MESH)

    def z_tail(q, t, owner):
        return pltpu.make_async_remote_copy(
            src_ref=z.at[LAST, pl.ds(*TAIL[q]), t], dst_ref=got.at[LATE - 1, pl.ds(*TAIL[q]), owner],
            send_sem=tsem.at[q, t], recv_sem=usem.at[q, owner], device_id=(1, t), device_id_type=MESH)

    def copies(rows, t, owner):
        return [z_copy(*r, t, owner) for r in rows] + [z_tail(q, t, owner) for q in range(len(TAIL))]

    barrier = pltpu.get_barrier_semaphore()

    def greet(where, targets):
        @pl.when(where)
        def _():
            for target in targets:
                pl.semaphore_signal(barrier, inc=1, device_id=target, device_id_type=MESH)

    greet(source & soon, [(1, 0), (1, 1), (1, 2), (1, 3), (0, lax.rem(tp + 2, TP))])
    greet(source & ~soon, [(1, LATER), (1, 2 + LATER)])
    greet(~source & soon, [(0, LATER), (0, 2 + LATER)])
    pl.semaphore_wait(barrier, jnp.where(source, jnp.where(soon, 1, 2), jnp.where(soon, 2, 4)))

    @pl.when(~source & soon)
    def _():
        for t in (SOON, 2 + SOON):
            pl.semaphore_signal(ready.at[0], inc=1, device_id=(0, t), device_id_type=MESH)

    @pl.when(~source & ~soon)
    def _():
        for t in range(TP):
            pl.semaphore_signal(ready.at[1], inc=1, device_id=(0, t), device_id_type=MESH)

    def sends(rows, k):
        for a in zip(*[copies(rows, t, tp) for t in (k, 2 + k)]):
            for c in a:
                c.start()

    chip, far = tp // 2, 1 - tp // 2

    @pl.when(source & soon)
    def _():
        pl.semaphore_wait(ready.at[0], 2)
        for c in copies(LATE_SOON, 2 * chip + SOON, tp):
            c.start()
        z_copy(*LATE_SOON[0], 2 * chip + SOON, tp).wait_send()
        for c in copies(LATE_SOON, 2 * far + SOON, tp):
            c.start()
        pl.semaphore_wait(ready.at[1], 2)
        sends(LATE_SOON, LATER)

    @pl.when(source & ~soon)
    def _():
        sends(LATE_LATER, SOON)
        pl.semaphore_wait(ready.at[1], 2)
        sends(LATE_LATER, LATER)

    @pl.when(source)
    def _():
        def clear(h, _):
            out[h] = jnp.zeros((W, CB, LANES), jnp.bfloat16)
            return 0
        lax.fori_loop(0, LATE, clear, 0)
        for rows, where in ((LATE_SOON, soon), (LATE_LATER, ~soon)):
            @pl.when(where)
            def _():
                for c in copies(rows[1:] if where is soon else rows, 2 * chip + SOON, tp):
                    c.wait_send()
                for t in (2 * chip + LATER, 2 * far, 2 * far + 1):
                    for c in copies(rows, t, tp):
                        c.wait_send()

    @pl.when(~source)
    def _():
        for s in (SOON, 2 + SOON):
            for piece in LATE_SOON:
                z_copy(*piece, s, s).wait_recv()

        def mixed(h, _):
            for p in range(PAIRS):
                parts = [got[h, p, s] if s % 2 == SOON else z[SPLIT + h, p, s] for s in range(TP)]
                turn(jnp.concatenate(parts, axis=0), out, h, p)
            return 0
        lax.fori_loop(0, LATER_SPLIT - SPLIT, mixed, 0)
        for first, rows in LATE_LATER:
            for s in range(TP):
                z_copy(first, rows, s, s).wait_recv()

            def row(h, _):
                for p in range(PAIRS):
                    turn(got[h, p].reshape(LANES, LANES), out, h, p)
                return 0
            lax.fori_loop(first, first + rows, row, 0)
        for q, (start, count) in enumerate(TAIL):
            for s in range(TP):
                z_tail(q, s, s).wait_recv()
            for p in range(start, start + count):
                turn(got[LATE - 1, p].reshape(LANES, LANES), out, LATE - 1, p)


def write(first, rows, each, src, *refs):
    dst, _, sem = refs[-3:]
    copies = [pltpu.make_async_copy(src.at[pl.ds(i * each, each)], dst.at[pl.ds(first + i * each, each)], sem.at[i])
              for i in range(rows // each)]
    for c in copies:
        c.start()
    for c in copies:
        c.wait()


def solution(mesh):
    def local_step(act, w, scale, shift):
        x = jnp.transpose(act, (1, 2, 0, 3))
        dma = pltpu.SemaphoreType.DMA
        shape = (H, W, CB, LANES)
        vmem, hbm = pl.BlockSpec(memory_space=pltpu.VMEM), pl.BlockSpec(memory_space=pl.ANY)
        early, z = pl.pallas_call(
            kernel,
            out_shape=(pltpu.VMEM((SPLIT, W, CB, LANES), jnp.bfloat16),
                       pltpu.VMEM((H, PAIRS, TP, N_LOC, LANES), jnp.bfloat16)),
            in_specs=[pl.BlockSpec(memory_space=pl.ANY), pl.BlockSpec(memory_space=pl.ANY),
                      pl.BlockSpec(memory_space=pl.ANY), pl.BlockSpec(memory_space=pl.ANY)],
            out_specs=(vmem, vmem),
            scratch_shapes=[
                pltpu.VMEM((H + 2, W + 2, N_LOC, C), jnp.bfloat16),
                pltpu.VMEM((2, 9, TP, C // TP, LANES), jnp.bfloat16),
                pltpu.VMEM((TP, 8, LANES), jnp.float32),
                dma((H,)), dma((2,)), dma((4, 3)), dma((4, TP)), dma((TP,)), dma((TP,)), dma((H, TP)), dma((H, TP)),
                dma((2, TP)), dma((2, TP)), pltpu.VMEM((2, 1, CB), jnp.float32), dma((2,)), pltpu.SemaphoreType.REGULAR,
            ],
            compiler_params=pltpu.CompilerParams(collective_id=0, has_side_effects=True, vmem_limit_bytes=42677043),
        )(x, w.reshape(9, C // TP, C), scale.reshape(1, CB), shift.reshape(1, CB))
        small = pltpu.CompilerParams(vmem_limit_bytes=2**20)
        written = (jax.ShapeDtypeStruct(shape, jnp.bfloat16), jax.ShapeDtypeStruct((8, LANES), jnp.float32))
        out, token = pl.pallas_call(
            functools.partial(write, 0, SPLIT, 1), out_shape=written, in_specs=[vmem], out_specs=(hbm, hbm), scratch_shapes=[dma((SPLIT // 1,))], compiler_params=small)(early)
        late = pl.pallas_call(
            finish,
            out_shape=pltpu.VMEM((LATE, W, CB, LANES), jnp.bfloat16),
            in_specs=[vmem, hbm],
            out_specs=vmem,
            scratch_shapes=[
                pltpu.VMEM((LATE, PAIRS, TP, N_LOC, LANES), jnp.bfloat16),
                dma((LATE, TP)), dma((LATE, TP)), dma((2, TP)), dma((2, TP)), pltpu.SemaphoreType.REGULAR((2,)),
            ],
            compiler_params=pltpu.CompilerParams(collective_id=1, has_side_effects=True, vmem_limit_bytes=12 * 2**20),
        )(z, token)
        out, _ = pl.pallas_call(
            functools.partial(write, SPLIT, LATE, 5), out_shape=written, in_specs=[vmem, hbm], out_specs=(hbm, hbm), scratch_shapes=[dma((LATE // 5,))], input_output_aliases={1: 0}, compiler_params=small)(late, out)
        return jnp.transpose(out, (3, 0, 1, 2))

    return jax.shard_map(local_step, mesh=mesh, in_specs=(P(("pp", "tp")), P(None, None, "tp", None), P("tp"), P("tp")),
                         out_specs=P("pp", None, None, "tp"), check_vma=False)
```
